32 devices in a mesh: gx: 2 (over x), gy: 4 (over y, core), gz: 4 (over z).
Axes of the slice: x: 2, y: 2, z: 4, core: 2. Of those that a mesh axis runs over, the one named last changes fastest.
Arguments:
- velocity: float32 [3, 32, 64, 1024], P(None, 'gx', 'gy', 'gz'), may hold values from -24 to 24
- metric: float32 [3, 32, 64, 1024], P(None, 'gx', 'gy', 'gz'), may hold values from 0.5 to 2
Outputs:
- viscosity: float32 [32, 64, 1024], P('gx', 'gy', 'gz')
- coefficient: float32 [32, 64], P('gx', 'gy')
The draws below stay inside these ranges and needn't reach their ends.
All inputs are finite; a program needn't handle non-finite values.
Results may differ from the reference program's by a relative error of at most 0.0003.
Values sent between devices are 32-bit elements; how exact they have to be, the bound alone decides.
A program may use at most 64 MiB of HBM per device.

```python
import math
import jax
import jax.numpy as jnp
from jax import lax

NX = 32
NY = 64
NZ = 1024


def draw_velocity(key, part):
    noise_key = jax.random.fold_in(key, 11)
    amplitude = 1.0 + 2.0 * jnp.arange(NZ, dtype=jnp.float32) / NZ
    random_part = jax.random.truncated_normal(noise_key, -4.0, 4.0, (3, NX, NY, NZ), jnp.float32)
    return random_part * amplitude


def block_scale(stream_key, dims, pieces, smallest, top_value):
    loudness = 1.0
    for dim, shards_of in pieces:
        heights = jax.random.uniform(jax.random.fold_in(jax.random.fold_in(stream_key, 6), dim), (shards_of,), jnp.float32, smallest / len(pieces), top_value / len(pieces))
        loudness = loudness * jnp.repeat(jnp.exp(heights), dims[dim] // shards_of).reshape((-1,) + (1,) * (len(dims) - 1 - dim))
    return loudness


def setup_inputs(seed: int = 0) -> dict:
    keys = jax.random.split(jax.random.key(seed), 3)
    return {
        "velocity": draw_velocity(jax.random.fold_in(keys[2], 71), 0),
        "metric": jnp.clip(jnp.exp(math.log(2.0) - 1.3862944 * jax.random.uniform(keys[1], (3, NX, NY, NZ), jnp.float32) ** block_scale(keys[1], (3, NX, NY, NZ), ((1, 2), (2, 4), (3, 4)), -0.2, 0.2)), 0.5, 2.0),
    }


pair_rows = (0, 1, 2, 0, 0, 1)
pair_cols = (0, 1, 2, 1, 2, 2)
pair_weight = (1.0, 1.0, 1.0, 2.0, 2.0, 2.0)
eps_line = 1e-06
ratio_square = 4.0

def pad_axis(values, axis_pos, periodic):
    length_axis = values.shape[axis_pos]
    if periodic:
        return jnp.concatenate([lax.slice_in_dim(values, length_axis - 1, length_axis, axis=axis_pos), values, lax.slice_in_dim(values, 0, 1, axis=axis_pos)], axis=axis_pos)
    widths = [(0, 0)] * values.ndim
    widths[axis_pos] = (1, 1)
    return jnp.pad(values, widths)

def box_three(padded, axis_pos):
    length_axis = padded.shape[axis_pos]
    lower_side = lax.slice_in_dim(padded, 0, length_axis - 2, axis=axis_pos)
    middle = lax.slice_in_dim(padded, 1, length_axis - 1, axis=axis_pos)
    upper_side = lax.slice_in_dim(padded, 2, length_axis, axis=axis_pos)
    return 0.25 * lower_side + 0.5 * middle + 0.25 * upper_side

def gradient_field(velocity_part, metric):
    columns = []
    for direction in range(3):
        padded = pad_axis(velocity_part, direction + 1, direction == 2)
        length_axis = padded.shape[direction + 1]
        differ = lax.slice_in_dim(padded, 2, length_axis, axis=direction + 1) - lax.slice_in_dim(padded, 0, length_axis - 2, axis=direction + 1)
        columns.append(0.5 * metric[direction] * differ)
    return jnp.stack(columns, axis=1)

def strain_parts(gradients):
    strain = 0.5 * (gradients + jnp.swapaxes(gradients, 0, 1))
    magnitude = jnp.sqrt(2.0 * lax.optimization_barrier(jnp.sum(strain * strain, axis=(0, 1))))
    strain_pairs = jnp.stack([strain[row_index, col_index] for row_index, col_index in zip(pair_rows, pair_cols)])
    return (strain_pairs, magnitude)

def make_fields(velocity_part, strain_pairs, magnitude):
    products = jnp.stack([velocity_part[row_index] * velocity_part[col_index] for row_index, col_index in zip(pair_rows, pair_cols)])
    return jnp.concatenate([velocity_part, products, magnitude[None] * strain_pairs], axis=0)

def germano(filtered, strain_hat, magnitude_hat, delta_sq):
    numerator = jnp.zeros_like(delta_sq)
    denominator = jnp.zeros_like(delta_sq)
    for position in range(6):
        row_index = pair_rows[position]
        col_index = pair_cols[position]
        leonard = filtered[3 + position] - filtered[row_index] * filtered[col_index]
        model_term = 2.0 * delta_sq * (filtered[9 + position] - ratio_square * magnitude_hat * strain_hat[position])
        numerator = numerator + pair_weight[position] * leonard * model_term
        denominator = denominator + pair_weight[position] * model_term * model_term
    return (numerator, denominator)

def reference(velocity, metric):
    delta_sq = (metric[0] * metric[1] * metric[2]) ** (-2.0 / 3.0)
    strain_pairs, magnitude = strain_parts(gradient_field(velocity, metric))
    fields = make_fields(velocity, strain_pairs, magnitude)
    filtered = box_three(pad_axis(fields, 1, False), 1)
    filtered = box_three(pad_axis(filtered, 2, False), 2)
    filtered = box_three(pad_axis(filtered, 3, True), 3)
    strain_hat, magnitude_hat = strain_parts(gradient_field(filtered[0:3], metric))
    numerator, denominator = germano(filtered, strain_hat, magnitude_hat, delta_sq)
    line_num = lax.optimization_barrier(jnp.sum(numerator, axis=2)) / NZ
    line_den = lax.optimization_barrier(jnp.sum(denominator, axis=2)) / NZ
    line_coef = line_num / (line_den + eps_line)
    peak_coef = jnp.max(line_coef)
    coefficient = jnp.minimum(line_coef, 0.5 * peak_coef)
    viscosity = coefficient[:, :, None] * delta_sq * magnitude
    return (viscosity, coefficient)
```

```python
import functools

import jax
import jax.numpy as jnp
from jax import lax
from jax.experimental import pallas as pl
from jax.experimental.pallas import tpu as pltpu
from jax.sharding import PartitionSpec as P

MESH = pl.DeviceIdType.MESH
pairs = ((0, 0), (1, 1), (2, 2), (0, 1), (0, 2), (1, 2))
eps_line = 1e-06
smallest = 1.1754944e-38
plane_offsets = [(dx, dy) for dx in (0, 1, -1) for dy in (0, 1, -1) if (dx, dy) != (0, 0)]
span_offsets = [(dx, dy, dz) for dz in (1, -1) for dx in (0, 1, -1) for dy in (0, 1, -1)]
G6 = 6


def root(s):
    return s * lax.rsqrt(jnp.maximum(s, smallest))


def tensor(d):
    f = [d[a][b] if a == b else d[a][b] + d[b][a] for a, b in pairs]
    square = (f[0] * f[0] + f[1] * f[1] + f[2] * f[2]) + 0.5 * (f[3] * f[3] + f[4] * f[4] + f[5] * f[5])
    return f, square


def model_sums(vv, ms, hat, dh, dq):
    f, square = tensor(dh)
    mh = root(8.0 * square)
    num = den = off = None
    for k, (a, b) in enumerate(pairs):
        leonard = vv[k] - hat[a] * hat[b]
        model = ms[k] - mh * f[k]
        n, m2 = leonard * model, model * model
        num = n if num is None else num + n
        if a == b:
            den = m2 if den is None else den + m2
        else:
            off = m2 if off is None else off + m2
    return num * dq, (den + 0.5 * off) * (dq * dq)


def kernel(sizes, vel, met, d_out, coef_out, V, Gv, G, H, Q, M, F, TE, E, EF, EG, PK, R, LS, PS, D, sem_in, send, recv, lsend, lrecv, psend, precv):
    NX, NY, NZ = sizes
    nx, ny, nz = vel.shape[1:]
    nt = nz // 128
    px = nx + 4
    starts = list(range(1, ny - 6, 8)) + [ny - 5]
    ix, iy, iz = lax.axis_index("gx"), lax.axis_index("gy"), lax.axis_index("gz")

    loads = []
    for k, src in enumerate((vel, met)):
        for t in range(nt):
            loads.append(pltpu.make_async_copy(
                src.at[:, :, :, 128 * t : 128 * t + 128],
                V.at[3 * k : 3 * k + 3, t, 2 : 2 + nx, 2 : 2 + ny, :],
                sem_in.at[k * nt + t]))
    for c in loads:
        c.start()

    def there(delta, i, n):
        return None if delta == 0 else (i + delta >= 0) & (i + delta < n)

    def exists(dx, dy):
        a, b = there(dx, ix, NX), there(dy, iy, NY)
        if a is None:
            return b
        return a if b is None else a & b

    def when(cond, fn):
        if cond is None:
            fn()
        else:
            pl.when(cond)(fn)

    def dev(d):
        return (ix + d[0], iy + d[1], lax.rem(iz + d[2] + NZ, NZ))

    barrier = pltpu.get_barrier_semaphore()
    expected = jnp.int32(0)
    for d in span_offsets + [(dx, dy, 0) for dx, dy in plane_offsets]:
        ok = exists(d[0], d[1])
        def sig(d=d):
            pl.semaphore_signal(barrier, inc=1, device_id=dev(d), device_id_type=MESH)
        when(ok, sig)
        expected = expected + (1 if ok is None else ok.astype(jnp.int32))
    for o in range(1, NZ):
        pl.semaphore_signal(barrier, inc=1, device_id=(ix, iy, lax.rem(iz + o, NZ)), device_id_type=MESH)
    plane_peers = [(a, b) for a in range(NX) for b in range(NY) if (a, b) != (0, 0)]
    for a, b in plane_peers:
        pl.semaphore_signal(barrier, inc=1, device_id=(lax.rem(ix + a, NX), lax.rem(iy + b, NY), iz), device_id_type=MESH)
    expected = expected + (NZ - 1 + len(plane_peers))

    z2 = jnp.zeros((2, 128), jnp.float32)
    for dx, p0 in ((-1, 0), (1, nx + 2)):
        def clear_planes(dx=dx, p0=p0):
            for f in range(6):
                for t in range(nt):
                    for p in (p0, p0 + 1):
                        V[f, t, p] = jnp.zeros((ny + 8, 128), jnp.float32)
            for s in range(2):
                for k in range(2):
                    R[s, dx + 1, k] = jnp.zeros((ny + 8, 128), jnp.float32)
        pl.when(jnp.logical_not(there(dx, ix, NX)))(clear_planes)
    for dy, r0 in ((-1, 0), (1, ny + 2)):
        def clear_rows(r0=r0):
            def body(p, _):
                for f in range(6):
                    for t in range(nt):
                        V[f, t, p, r0 : r0 + 2, :] = z2
                return 0
            lax.fori_loop(0, px, body, 0)
            for s in range(2):
                for f in range(6):
                    TE[s, f, r0 : r0 + 2, :] = z2
                for dxi in range(3):
                    for k in range(2):
                        R[s, dxi, k, r0 : r0 + 2, :] = z2
        pl.when(jnp.logical_not(there(dy, iy, NY)))(clear_rows)

    for c in loads:
        c.wait()

    lane = lax.broadcasted_iota(jnp.int32, (ny, 128), 1)
    group = (lane * 43) >> 8
    inner = lane - G6 * group
    lane8, group8, inner8 = lane[0:8], group[0:8], inner[0:8]

    def lroll(a, s):
        s = s % 128
        return pltpu.roll(a, s, 1) if s else a

    for f in range(6):
        for s in range(2):
            acc = jnp.zeros((ny, 128), jnp.float32)
            for p in range(2, 2 + nx):
                tile = V[f, 0 if s == 0 else nt - 1, p, 2 : 2 + ny, :]
                acc = jnp.where(group == p, lroll(tile, G6 * p - (0 if s == 0 else 122)), acc)
            TE[s, f, 2 : 2 + ny, :] = acc
    for s in range(2):
        for k in range(2):
            parts = [lroll(TE[s, 3 * k + c, 2 : 2 + ny, :], 2 * c - (0 if s == 0 else 4)) for c in range(3)]
            PK[s, k] = jnp.where(inner < 2, parts[0], jnp.where(inner < 4, parts[1], parts[2]))

    pl.semaphore_wait(barrier, expected)

    def span_x(dx, deep):
        if dx == 0:
            return (2, 2, nx)
        if dx == 1:
            return (nx, 0, 2) if deep else (nx + 1, 1, 1)
        return (2, nx + 2, 2) if deep else (2, nx + 2, 1)

    def span_y(dy, deep):
        if dy == 0:
            return (2, 2, ny)
        if dy == 1:
            return (ny, 0, 2) if deep else (ny + 1, 1, 1)
        return (2, ny + 2, 2) if deep else (2, ny + 2, 1)

    def remote(src, dst, j, d):
        return pltpu.make_async_remote_copy(src_ref=src, dst_ref=dst, send_sem=send.at[j], recv_sem=recv.at[j], device_id=dev(d), device_id_type=MESH)

    def span_copy(n):
        dx, dy, dz = d = span_offsets[n]
        s = 1 if dz == 1 else 0
        ys, yd, yn = span_y(dy, True)
        return remote(PK.at[s, :, ys - 2 : ys - 2 + yn, :], R.at[s, 1 - dx, :, yd : yd + yn, :], n, d)

    def plane_copies(n):
        dx, dy = plane_offsets[n]
        d = (dx, dy, 0)
        base = len(span_offsets) + 3 * n
        out = []
        for k in range(2):
            xs, xd, xn = span_x(dx, k == 0)
            ys, yd, yn = span_y(dy, k == 0)
            f0 = 3 * k
            out.append(remote(V.at[f0 : f0 + 3, :, xs : xs + xn, ys : ys + yn, :], V.at[f0 : f0 + 3, :, xd : xd + xn, yd : yd + yn, :], base + k, d))
        if dx == 0:
            ys, yd, yn = span_y(dy, True)
            out.append(remote(TE.at[:, :, ys : ys + yn, :], TE.at[:, :, yd : yd + yn, :], base + 2, d))
        return out

    everything = [(d, (lambda n=n: [span_copy(n)])) for n, d in enumerate(span_offsets)]
    everything += [((dx, dy, 0), (lambda n=n: plane_copies(n))) for n, (dx, dy) in enumerate(plane_offsets)]
    for d, make in everything:
        def go(make=make):
            for c in make():
                c.start()
        when(exists(d[0], d[1]), go)

    def land(wanted):
        for d, make in everything:
            if wanted(d):
                def arrive(make=make):
                    for c in make():
                        c.wait_recv()
                when(exists(-d[0], -d[1]), arrive)

    first, last = lane8 == 0, lane8 == 127

    def zup(a):
        r = [pltpu.roll(v, 127, 1) for v in a]
        return [jnp.where(last, r[(t + 1) % nt], r[t]) for t in range(nt)]

    def zdown(a):
        r = [pltpu.roll(v, 1, 1) for v in a]
        return [jnp.where(first, r[t - 1], r[t]) for t in range(nt)]

    def zsmooth(a):
        t1 = [v + w for v, w in zip(a, zup(a))]
        return [v + w for v, w in zip(t1, zdown(t1))]

    def field_plane(x, _):
        for r in starts:
            here = slice(r, r + 8)
            m = [[V[3 + c, t, x, here, :] for c in range(3)] for t in range(nt)]
            u, d = [], [[[None] * 3 for _ in range(3)] for _ in range(nt)]
            for i in range(3):
                mid = [V[i, t, x, here, :] for t in range(nt)]
                u.append(mid)
                hi, lo = zup(mid), zdown(mid)
                for t in range(nt):
                    above, below = V[i, t, x, r + 1 : r + 9, :], V[i, t, x, r - 1 : r + 7, :]
                    Gv[i, t, x, here, :] = (mid[t] + mid[t]) + (above + below)
                    d[t][i][0] = m[t][0] * (V[i, t, x + 1, here, :] - V[i, t, x - 1, here, :])
                    d[t][i][1] = m[t][1] * (above - below)
                    d[t][i][2] = m[t][2] * (hi[t] - lo[t])
            for t in range(nt):
                f, square = tensor(d[t])
                mag = root(0.5 * square)
                dq = jnp.exp2((-2.0 / 3.0) * jnp.log2(m[t][0] * m[t][1] * m[t][2]))
                Q[t, x, here, :] = dq
                M[t, x, here, :] = dq * mag
                for k, (a, b) in enumerate(pairs):
                    F[k, t, x, here, :] = u[a][t] * u[b][t]
                    F[6 + k, t, x, here, :] = mag * f[k]
        return 0

    def velocity_plane(x, _):
        for c in range(3):
            for t in range(nt):
                for r in starts:
                    mid = V[c, t, x, r : r + 8, :]
                    Gv[c, t, x, r : r + 8, :] = (mid + mid) + (V[c, t, x, r - 1 : r + 7, :] + V[c, t, x, r + 1 : r + 9, :])
        return 0

    def smooth_plane(x, _):
        for k in range(12):
            for t in range(nt):
                for r in range(0, ny, 8):
                    mid = F[k, t, x, r + 2 : r + 10, :]
                    G[k, t, x, r : r + 8, :] = (mid + mid) + (F[k, t, x, r + 1 : r + 9, :] + F[k, t, x, r + 3 : r + 11, :])
        return 0

    has_lo = jnp.where(iy > 0, 0.125, 0.0)
    has_hi = jnp.where(iy < NY - 1, 0.125, 0.0)
    rows8 = lax.broadcasted_iota(jnp.int32, (8, 128), 0)

    def row_scale(r):
        idx = rows8 + r
        return jnp.where(idx < 2, has_lo, jnp.where(idx < ny + 2, 0.125, has_hi))

    def hat_plane(x, _):
        inside = jnp.where((x == 1) & (ix == 0), 0.0, jnp.where((x == nx + 2) & (ix == NX - 1), 0.0, 1.0))
        for r in starts:
            scale = row_scale(r) * inside
            for c in range(3):
                s = []
                for t in range(nt):
                    mid = Gv[c, t, x, r : r + 8, :]
                    s.append((mid + mid) + (Gv[c, t, x - 1, r : r + 8, :] + Gv[c, t, x + 1, r : r + 8, :]))
                s = zsmooth(s)
                for t in range(nt):
                    H[c, t, x, r : r + 8, :] = s[t] * scale
        return 0

    keep = [None] * nt
    keep[0] = lane8 >= 2
    keep[nt - 1] = (lane8 < 126) if nt > 1 else (lane8 >= 2) & (lane8 < 126)

    def line_plane(x, sums):
        out = []
        for b, r in enumerate(range(0, ny, 8)):
            here = slice(r + 2, r + 10)
            filtered = []
            for k in range(12):
                s = []
                for t in range(nt):
                    mid = G[k, t, x, r : r + 8, :]
                    s.append((mid + mid) + (G[k, t, x - 1, r : r + 8, :] + G[k, t, x + 1, r : r + 8, :]))
                filtered.append(zsmooth(s))
            hat, d = [], [[[None] * 3 for _ in range(3)] for _ in range(nt)]
            m = [[V[3 + c, t, x, here, :] for c in range(3)] for t in range(nt)]
            for i in range(3):
                mid = [H[i, t, x, here, :] for t in range(nt)]
                hat.append(mid)
                hi, lo = zup(mid), zdown(mid)
                for t in range(nt):
                    d[t][i][0] = m[t][0] * (H[i, t, x + 1, here, :] - H[i, t, x - 1, here, :])
                    d[t][i][1] = m[t][1] * (H[i, t, x, r + 3 : r + 11, :] - H[i, t, x, r + 1 : r + 9, :])
                    d[t][i][2] = m[t][2] * (hi[t] - lo[t])
            num = den = 0.0
            for t in range(nt):
                n, e = model_sums([filtered[k][t] for k in range(6)], [filtered[6 + k][t] for k in range(6)], [h[t] for h in hat], d[t], Q[t, x, here, :])
                if keep[t] is not None:
                    n, e = jnp.where(keep[t], n, 0.0), jnp.where(keep[t], e, 0.0)
                num, den = num + n, den + e
            num = jnp.sum(num, axis=1, keepdims=True)
            den = jnp.sum(den, axis=1, keepdims=True)
            acc = jnp.where(lane8 == G6 * x + 2, num, sums[b])
            out.append(jnp.where(lane8 == G6 * x + 4, den, acc))
        return tuple(out)

    land(lambda d: d[0] == 0 and d[2] == 0)
    lax.fori_loop(3, nx + 1, field_plane, 0, unroll=2)
    lax.fori_loop(0, 2, lambda i, c: velocity_plane(2 + i * (nx - 1), c), 0)
    lax.fori_loop(3, nx + 1, smooth_plane, 0, unroll=2)
    lax.fori_loop(3, nx + 1, hat_plane, 0, unroll=2)
    sums = tuple(jnp.zeros((8, 128), jnp.float32) for _ in range(0, ny, 8))
    sums = lax.fori_loop(4, nx, line_plane, sums)
    land(lambda d: d[0] != 0 and d[2] == 0)

    def edges(per_side):
        return lambda i: jnp.where(i < len(per_side), per_side[0] + i, nx + 3 - per_side[-1] + i - len(per_side))
    near, inner_planes = edges([1, 2]), edges([2, 3])
    lax.fori_loop(0, 4, lambda i, c: field_plane(near(i), c), 0)
    lax.fori_loop(0, 2, lambda i, c: velocity_plane(i * (nx + 3), c), 0)
    lax.fori_loop(0, 4, lambda i, c: smooth_plane(near(i), c), 0)
    lax.fori_loop(0, 4, lambda i, c: hat_plane(near(i), c), 0)
    sums = lax.fori_loop(0, 4, lambda i, c: line_plane(inner_planes(i), c), sums)
    land(lambda d: d[2] != 0)

    yr = ny + 8
    lane_r = lax.broadcasted_iota(jnp.int32, (yr, 128), 1)
    group_r = (lane_r * 43) >> 8
    inner_r = lane_r - G6 * group_r
    rows_r = lax.broadcasted_iota(jnp.int32, (yr, 128), 0)
    outside = ((group_r == 1) & (ix == 0)) | ((group_r == nx + 2) & (ix == NX - 1))
    outside = outside | ((rows_r < 2) & (iy == 0)) | ((rows_r >= ny + 2) & (iy == NY - 1))
    scale_r = jnp.where(outside, 0.0, 0.125)
    enum, eden = 0.0, 0.0
    fixes = []
    for s in range(2):
        mixed = []
        for k in range(2):
            far = jnp.where(lane_r < 2 * G6, lroll(R[1 - s, 0, k], -G6 * nx), R[1 - s, 1, k])
            mixed.append(jnp.where(lane_r >= G6 * (nx + 2), lroll(R[1 - s, 2, k], G6 * nx), far))
        fields = []
        for f in range(6):
            own = TE[s, f]
            for p in (0, 1, nx + 2, nx + 3):
                if f >= 3 and p in (0, nx + 3):
                    continue
                tile = V[f, 0 if s == 0 else nt - 1, p]
                own = jnp.where(group_r == p, lroll(tile, G6 * p - (0 if s == 0 else 122)), own)
            c = f % 3
            if s == 0:
                fields.append(jnp.where(inner_r < 2, lroll(mixed[f // 3], -2 * c), lroll(own, 2)))
            else:
                fields.append(jnp.where(inner_r >= 4, lroll(mixed[f // 3], 4 - 2 * c), lroll(own, -2)))
        u, m = fields[0:3], fields[3:6]
        for f in range(6):
            E[s, f] = fields[f]
        def shift(a, n):
            return lroll(a, -n)
        d = [[None] * 3 for _ in range(3)]
        for i in range(3):
            d[i][0] = m[0] * (shift(u[i], G6) - shift(u[i], -G6))
            d[i][1] = m[1] * (pltpu.roll(u[i], yr - 1, 0) - pltpu.roll(u[i], 1, 0))
            d[i][2] = m[2] * (shift(u[i], 1) - shift(u[i], -1))
        f, square = tensor(d)
        mag = root(0.5 * square)
        dq = jnp.exp2((-2.0 / 3.0) * jnp.log2(m[0] * m[1] * m[2]))
        EF[s, 15] = dq
        EF[s, 16] = dq * mag
        for c in range(3):
            EF[s, 12 + c] = u[c]
        for k, (a, b) in enumerate(pairs):
            EF[s, k] = u[a] * u[b]
            EF[s, 6 + k] = mag * f[k]
        def lanes_smooth(a):
            b = (a + a) + (shift(a, G6) + shift(a, -G6))
            return (b + b) + (shift(b, 1) + shift(b, -1))
        for c in range(3):
            y = (u[c] + u[c]) + (pltpu.roll(u[c], yr - 1, 0) + pltpu.roll(u[c], 1, 0))
            EG[s, c] = lanes_smooth(y) * scale_r
        own = slice(2, 2 + ny)
        filtered = []
        for k in range(12):
            mid = EF[s, k, own, :]
            filtered.append(lanes_smooth((mid + mid) + (EF[s, k, 1 : 1 + ny, :] + EF[s, k, 3 : 3 + ny, :])))
        hat, dh = [], [[None] * 3 for _ in range(3)]
        me = [E[s, 3 + c, own, :] for c in range(3)]
        for i in range(3):
            mid = EG[s, i, own, :]
            hat.append(mid)
            dh[i][0] = me[0] * (shift(mid, G6) - shift(mid, -G6))
            dh[i][1] = me[1] * (EG[s, i, 3 : 3 + ny, :] - EG[s, i, 1 : 1 + ny, :])
            dh[i][2] = me[2] * (shift(mid, 1) - shift(mid, -1))
        n, e = model_sums(filtered[0:6], filtered[6:12], hat, dh, EF[s, 15, own, :])
        enum, eden = enum + n, eden + e
    enum = enum + lroll(enum, -1)
    eden = lroll(eden + lroll(eden, -1), 2)
    used = (group >= 2) & (group < nx + 2)
    extra = jnp.where(used & (inner == 2), enum, jnp.where(used & (inner == 4), eden, 0.0))
    LS[iz] = jnp.concatenate(sums, axis=0) + extra

    def line_copy(o):
        return pltpu.make_async_remote_copy(
            src_ref=LS.at[iz], dst_ref=LS.at[iz], send_sem=lsend.at[o - 1], recv_sem=lrecv.at[o - 1],
            device_id=(ix, iy, lax.rem(iz + o, NZ)), device_id_type=MESH)
    def line_landing(o):
        src = lax.rem(iz - o + NZ, NZ)
        return pltpu.make_async_remote_copy(
            src_ref=LS.at[src], dst_ref=LS.at[src], send_sem=lsend.at[o - 1], recv_sem=lrecv.at[o - 1],
            device_id=(ix, iy, lax.rem(iz + o, NZ)), device_id_type=MESH)
    for o in range(1, NZ):
        line_copy(o).start()

    lo_fix, hi_fix = EF[0, 16, 2 : 2 + ny, :], EF[1, 16, 2 : 2 + ny, :]
    for x in range(nx):
        p = x + 2
        for t in range(nt):
            tile = M[t, p, 2 : 2 + ny, :]
            if t == 0:
                tile = jnp.where(lane == 0, lroll(lo_fix, -(G6 * p + 2)), tile)
            if t == nt - 1:
                tile = jnp.where(lane == 127, lroll(hi_fix, 127 - (G6 * p + 3)), tile)
            D[x, :, 128 * t : 128 * t + 128] = tile
    save = pltpu.make_async_copy(D, d_out, sem_in.at[2 * nt])
    save.start()

    for o in range(1, NZ):
        line_landing(o).wait_recv()
    total = LS[0]
    for o in range(1, NZ):
        total = total + LS[o]
    unit = 4096.0 * nz * NZ
    coef = (total / unit) / (lroll(total, -2) / unit + eps_line)
    masked = jnp.where(used & (inner == 2), coef, -jnp.inf)
    here_max = masked[0:8]
    for r in range(8, ny, 8):
        here_max = jnp.maximum(here_max, masked[r : r + 8])
    me = ix * NY + iy
    PS[me] = here_max
    def peak_copy(j, a, b, landing):
        tx, ty = lax.rem(ix + a, NX), lax.rem(iy + b, NY)
        slot = me
        if landing:
            slot = lax.rem(ix - a + NX, NX) * NY + lax.rem(iy - b + NY, NY)
        return pltpu.make_async_remote_copy(
            src_ref=PS.at[slot], dst_ref=PS.at[slot], send_sem=psend.at[j], recv_sem=precv.at[j],
            device_id=(tx, ty, iz), device_id_type=MESH)
    for j, (a, b) in enumerate(plane_peers):
        peak_copy(j, a, b, False).start()
    for o in range(1, NZ):
        line_copy(o).wait_send()
    for d, make in everything:
        def left(make=make):
            for c in make():
                c.wait_send()
        when(exists(d[0], d[1]), left)
    for j, (a, b) in enumerate(plane_peers):
        peak_copy(j, a, b, True).wait_recv()
    peak = PS[0]
    for j in range(1, NX * NY):
        peak = jnp.maximum(peak, PS[j])
    coef_out[...] = jnp.minimum(coef, 0.5 * jnp.max(peak, axis=(0, 1), keepdims=True))
    save.wait()
    for j, (a, b) in enumerate(plane_peers):
        peak_copy(j, a, b, False).wait_send()


def scale_kernel(D, coef, visc, coef_out):
    nx, ny = visc.shape[:2]
    lane = lax.broadcasted_iota(jnp.int32, (ny, 128), 1)
    table = coef[...]
    turned = table.T
    for x in range(nx):
        at = G6 * (x + 2) + 2
        column = jnp.sum(jnp.where(lane == at, table, 0.0), axis=1, keepdims=True)
        visc[x] = D[x] * column
        coef_out[x : x + 1, :] = turned[at : at + 1, :]


def per_device(sizes, velocity, metric):
    nx, ny, nz = velocity.shape[1:]
    NX, NY, NZ = sizes
    assert nz % 128 == 0 and ny % 8 == 0 and G6 * (nx + 4) <= 128 and nx >= 6
    nt, px, yr = nz // 128, nx + 4, ny + 8
    f32 = jnp.float32
    copies = len(span_offsets) + 3 * len(plane_offsets)
    dmag, coef = pl.pallas_call(
        functools.partial(kernel, sizes),
        out_shape=(jax.ShapeDtypeStruct((nx, ny, nz), f32), jax.ShapeDtypeStruct((ny, 128), f32)),
        in_specs=[pl.BlockSpec(memory_space=pltpu.HBM)] * 2,
        out_specs=(pl.BlockSpec(memory_space=pltpu.HBM), pl.BlockSpec(memory_space=pltpu.VMEM)),
        scratch_shapes=[
            pltpu.VMEM((6, nt, px, yr, 128), f32),
            pltpu.VMEM((3, nt, px, yr, 128), f32),
            pltpu.VMEM((12, nt, px, ny, 128), f32),
            pltpu.VMEM((3, nt, px, yr, 128), f32),
            pltpu.VMEM((nt, px, yr, 128), f32),
            pltpu.VMEM((nt, px, yr, 128), f32),
            pltpu.VMEM((12, nt, px, yr, 128), f32),
            pltpu.VMEM((2, 6, yr, 128), f32),
            pltpu.VMEM((2, 6, yr, 128), f32),
            pltpu.VMEM((2, 17, yr, 128), f32),
            pltpu.VMEM((2, 3, yr, 128), f32),
            pltpu.VMEM((2, 2, ny, 128), f32),
            pltpu.VMEM((2, 3, 2, yr, 128), f32),
            pltpu.VMEM((NZ, ny, 128), f32),
            pltpu.VMEM((NX * NY, 8, 128), f32),
            pltpu.VMEM((nx, ny, nz), f32),
            pltpu.SemaphoreType.DMA((2 * nt + 1,)),
            pltpu.SemaphoreType.DMA((copies,)),
            pltpu.SemaphoreType.DMA((copies,)),
            pltpu.SemaphoreType.DMA((NZ,)),
            pltpu.SemaphoreType.DMA((NZ,)),
            pltpu.SemaphoreType.DMA((NX * NY,)),
            pltpu.SemaphoreType.DMA((NX * NY,)),
        ],
        compiler_params=pltpu.CompilerParams(collective_id=0, has_side_effects=True, vmem_limit_bytes=67043328 - 600 * 1024),
    )(velocity, metric)
    return pl.pallas_call(
        scale_kernel,
        out_shape=(jax.ShapeDtypeStruct((nx, ny, nz), f32), jax.ShapeDtypeStruct((nx, ny), f32)),
        in_specs=[pl.BlockSpec(memory_space=pltpu.VMEM)] * 2,
        out_specs=(pl.BlockSpec(memory_space=pltpu.VMEM),) * 2,
        compiler_params=pltpu.CompilerParams(vmem_limit_bytes=4 * 1024 * 1024),
    )(dmag, coef)


def solution(mesh):
    sizes = (mesh.shape["gx"], mesh.shape["gy"], mesh.shape["gz"])
    return jax.shard_map(
        functools.partial(per_device, sizes),
        mesh=mesh,
        in_specs=(P(None, "gx", "gy", "gz"), P(None, "gx", "gy", "gz")),
        out_specs=(P("gx", "gy", "gz"), P("gx", "gy")),
        check_vma=False,
    )
```

```python
import functools

import jax
import jax.numpy as jnp
from jax import lax
from jax.experimental import pallas as pl
from jax.experimental.pallas import tpu as pltpu
from jax.sharding import PartitionSpec as P

MESH = pl.DeviceIdType.MESH
pairs = ((0, 0), (1, 1), (2, 2), (0, 1), (0, 2), (1, 2))
eps_line = 1e-06
smallest = 1.1754944e-38
plane_offsets = [(dx, dy) for dx in (0, 1, -1) for dy in (0, 1, -1) if (dx, dy) != (0, 0)]
span_offsets = [(dx, dy, dz) for dz in (1, -1) for dx in (0, 1, -1) for dy in (0, 1, -1)]
chunks = 4
G6 = 6


def root(s):
    return s * lax.rsqrt(jnp.maximum(s, smallest))


def tensor(d):
    f = [d[a][b] if a == b else d[a][b] + d[b][a] for a, b in pairs]
    square = (f[0] * f[0] + f[1] * f[1] + f[2] * f[2]) + 0.5 * (f[3] * f[3] + f[4] * f[4] + f[5] * f[5])
    return f, square


def model_sums(vv, ms, hat, dh, dq):
    f, square = tensor(dh)
    mh = root(8.0 * square)
    num = den = off = None
    for k, (a, b) in enumerate(pairs):
        leonard = vv[k] - hat[a] * hat[b]
        model = ms[k] - mh * f[k]
        n, m2 = leonard * model, model * model
        num = n if num is None else num + n
        if a == b:
            den = m2 if den is None else den + m2
        else:
            off = m2 if off is None else off + m2
    return num * dq, (den + 0.5 * off) * (dq * dq)


def kernel(sizes, vel, met, d_out, coef_out, V, Gv, G, H, Q, M, F, TE, E, EF, EG, PK, R, LS, PS, D, W, sem_in, send, recv, lsend, lrecv, psend, precv):
    NX, NY, NZ = sizes
    nx, ny, nz = vel.shape[1:]
    nt = nz // 128
    px = nx + 4
    starts = list(range(1, ny - 6, 8)) + [ny - 5]
    ix, iy, iz = lax.axis_index("gx"), lax.axis_index("gy"), lax.axis_index("gz")

    loads = []
    for k, src in enumerate((vel, met)):
        for t in range(nt):
            loads.append(pltpu.make_async_copy(
                src.at[:, :, :, 128 * t : 128 * t + 128],
                V.at[3 * k : 3 * k + 3, t, 2 : 2 + nx, 2 : 2 + ny, :],
                sem_in.at[k * nt + t]))
    for c in loads:
        c.start()

    def there(delta, i, n):
        return None if delta == 0 else (i + delta >= 0) & (i + delta < n)

    def exists(dx, dy):
        a, b = there(dx, ix, NX), there(dy, iy, NY)
        if a is None:
            return b
        return a if b is None else a & b

    def when(cond, fn):
        if cond is None:
            fn()
        else:
            pl.when(cond)(fn)

    def dev(d):
        return (ix + d[0], iy + d[1], lax.rem(iz + d[2] + NZ, NZ))

    barrier = pltpu.get_barrier_semaphore()
    expected = jnp.int32(0)
    for d in span_offsets + [(dx, dy, 0) for dx, dy in plane_offsets]:
        ok = exists(d[0], d[1])
        def sig(d=d):
            pl.semaphore_signal(barrier, inc=1, device_id=dev(d), device_id_type=MESH)
        when(ok, sig)
        expected = expected + (1 if ok is None else ok.astype(jnp.int32))
    for o in range(1, NZ):
        pl.semaphore_signal(barrier, inc=1, device_id=(ix, iy, lax.rem(iz + o, NZ)), device_id_type=MESH)
    plane_peers = [(a, b) for a in range(NX) for b in range(NY) if (a, b) != (0, 0)]
    for a, b in plane_peers:
        pl.semaphore_signal(barrier, inc=1, device_id=(lax.rem(ix + a, NX), lax.rem(iy + b, NY), iz), device_id_type=MESH)
    expected = expected + (NZ - 1 + len(plane_peers))

    z2 = jnp.zeros((2, 128), jnp.float32)
    for dx, p0 in ((-1, 0), (1, nx + 2)):
        def clear_planes(dx=dx, p0=p0):
            for f in range(6):
                for t in range(nt):
                    for p in (p0, p0 + 1):
                        V[f, t, p] = jnp.zeros((ny + 8, 128), jnp.float32)
            for s in range(2):
                for k in range(2):
                    R[s, dx + 1, k] = jnp.zeros((ny + 8, 128), jnp.float32)
        pl.when(jnp.logical_not(there(dx, ix, NX)))(clear_planes)
    for dy, r0 in ((-1, 0), (1, ny + 2)):
        def clear_rows(r0=r0):
            def body(p, _):
                for f in range(6):
                    for t in range(nt):
                        V[f, t, p, r0 : r0 + 2, :] = z2
                return 0
            lax.fori_loop(0, px, body, 0)
            for s in range(2):
                for f in range(6):
                    TE[s, f, r0 : r0 + 2, :] = z2
                for dxi in range(3):
                    for k in range(2):
                        R[s, dxi, k, r0 : r0 + 2, :] = z2
        pl.when(jnp.logical_not(there(dy, iy, NY)))(clear_rows)

    for c in loads:
        c.wait()

    lane = lax.broadcasted_iota(jnp.int32, (ny, 128), 1)
    group = (lane * 43) >> 8
    inner = lane - G6 * group
    lane8, group8, inner8 = lane[0:8], group[0:8], inner[0:8]

    def lroll(a, s):
        s = s % 128
        return pltpu.roll(a, s, 1) if s else a

    for f in range(6):
        for s in range(2):
            acc = jnp.zeros((ny, 128), jnp.float32)
            for p in range(2, 2 + nx):
                tile = V[f, 0 if s == 0 else nt - 1, p, 2 : 2 + ny, :]
                acc = jnp.where(group == p, lroll(tile, G6 * p - (0 if s == 0 else 122)), acc)
            TE[s, f, 2 : 2 + ny, :] = acc
    for s in range(2):
        for k in range(2):
            parts = [lroll(TE[s, 3 * k + c, 2 : 2 + ny, :], 2 * c - (0 if s == 0 else 4)) for c in range(3)]
            PK[s, k] = jnp.where(inner < 2, parts[0], jnp.where(inner < 4, parts[1], parts[2]))

    pl.semaphore_wait(barrier, expected)

    def span_x(dx, deep):
        if dx == 0:
            return (2, 2, nx)
        if dx == 1:
            return (nx, 0, 2) if deep else (nx + 1, 1, 1)
        return (2, nx + 2, 2) if deep else (2, nx + 2, 1)

    def span_y(dy, deep):
        if dy == 0:
            return (2, 2, ny)
        if dy == 1:
            return (ny, 0, 2) if deep else (ny + 1, 1, 1)
        return (2, ny + 2, 2) if deep else (2, ny + 2, 1)

    def remote(src, dst, j, d):
        return pltpu.make_async_remote_copy(src_ref=src, dst_ref=dst, send_sem=send.at[j], recv_sem=recv.at[j], device_id=dev(d), device_id_type=MESH)

    def span_copy(n):
        dx, dy, dz = d = span_offsets[n]
        s = 1 if dz == 1 else 0
        ys, yd, yn = span_y(dy, True)
        return remote(PK.at[s, :, ys - 2 : ys - 2 + yn, :], R.at[s, 1 - dx, :, yd : yd + yn, :], n, d)

    chunk = nx // chunks

    def plane_copies(n, part=None):
        dx, dy = plane_offsets[n]
        d = (dx, dy, 0)
        base = len(span_offsets) + (2 * chunks + 1) * n
        out = []
        for c in range(chunks if dx == 0 else 1):
            if part is not None and c != part:
                continue
            for k in range(2):
                xs, xd, xn = span_x(dx, k == 0)
                if dx == 0:
                    xs, xd, xn = 2 + c * chunk, 2 + c * chunk, chunk
                ys, yd, yn = span_y(dy, k == 0)
                f0 = 3 * k
                out.append(remote(V.at[f0 : f0 + 3, :, xs : xs + xn, ys : ys + yn, :], V.at[f0 : f0 + 3, :, xd : xd + xn, yd : yd + yn, :], base + 2 * c + k, d))
        if dx == 0 and part in (None, chunks - 1):
            ys, yd, yn = span_y(dy, True)
            out.append(remote(TE.at[:, :, ys : ys + yn, :], TE.at[:, :, yd : yd + yn, :], base + 2 * chunks, d))
        return out

    everything = [(d, (lambda n=n: [span_copy(n)])) for n, d in enumerate(span_offsets)]
    everything += [((dx, dy, 0), (lambda n=n: plane_copies(n))) for n, (dx, dy) in enumerate(plane_offsets)]
    for d, make in everything:
        def go(make=make):
            for c in make():
                c.start()
        when(exists(d[0], d[1]), go)

    def land(wanted):
        for d, make in everything:
            if wanted(d):
                def arrive(make=make):
                    for c in make():
                        c.wait_recv()
                when(exists(-d[0], -d[1]), arrive)

    first, last = lane8 == 0, lane8 == 127

    def zup(a):
        r = [pltpu.roll(v, 127, 1) for v in a]
        return [jnp.where(last, r[(t + 1) % nt], r[t]) for t in range(nt)]

    def zdown(a):
        r = [pltpu.roll(v, 1, 1) for v in a]
        return [jnp.where(first, r[t - 1], r[t]) for t in range(nt)]

    def zsmooth(a):
        return [(v + v) + (w + q) for v, w, q in zip(a, zup(a), zdown(a))]

    def field_plane(x, _):
        for r in starts:
            here = slice(r, r + 8)
            m = [[V[3 + c, t, x, here, :] for c in range(3)] for t in range(nt)]
            u, d = [], [[[None] * 3 for _ in range(3)] for _ in range(nt)]
            for i in range(3):
                mid = [V[i, t, x, here, :] for t in range(nt)]
                u.append(mid)
                hi, lo = zup(mid), zdown(mid)
                for t in range(nt):
                    above, below = V[i, t, x, r + 1 : r + 9, :], V[i, t, x, r - 1 : r + 7, :]
                    Gv[i, t, x, here, :] = (mid[t] + mid[t]) + (above + below)
                    d[t][i][0] = m[t][0] * (V[i, t, x + 1, here, :] - V[i, t, x - 1, here, :])
                    d[t][i][1] = m[t][1] * (above - below)
                    d[t][i][2] = m[t][2] * (hi[t] - lo[t])
            for t in range(nt):
                f, square = tensor(d[t])
                mag = root(0.5 * square)
                dq = jnp.exp2((-2.0 / 3.0) * jnp.log2(m[t][0] * m[t][1] * m[t][2]))
                Q[t, x, here, :] = dq
                M[t, x, here, :] = dq * mag
                for k, (a, b) in enumerate(pairs):
                    F[k, t, x, here, :] = u[a][t] * u[b][t]
                    F[6 + k, t, x, here, :] = mag * f[k]
        return 0

    def velocity_plane(x, _):
        for c in range(3):
            for t in range(nt):
                for r in starts:
                    mid = V[c, t, x, r : r + 8, :]
                    Gv[c, t, x, r : r + 8, :] = (mid + mid) + (V[c, t, x, r - 1 : r + 7, :] + V[c, t, x, r + 1 : r + 9, :])
        return 0

    zi = lax.broadcasted_iota(jnp.int32, (nz, nz), 0)
    zj = lax.broadcasted_iota(jnp.int32, (nz, nz), 1)
    gap = jnp.abs(zi - zj)
    W[...] = jnp.where(gap == 0, 2.0, jnp.where((gap == 1) | (gap == nz - 1), 1.0, 0.0)).astype(jnp.bfloat16)

    def banded(a):
        w = W[...]
        hi = a.astype(jnp.bfloat16)
        rest = a - hi.astype(jnp.float32)
        mid = rest.astype(jnp.bfloat16)
        low = (rest - mid.astype(jnp.float32)).astype(jnp.bfloat16)
        n = a.shape[0]
        out = jnp.dot(jnp.concatenate([hi, mid, low], axis=0), w, preferred_element_type=jnp.float32)
        return out[0:n] + (out[n : 2 * n] + out[2 * n :])

    def smooth_plane(x, _):
        for k0 in (0,):
            s = []
            for k in range(12):
                row = []
                for t in range(nt):
                    mid = F[k, t, x, 2 : 2 + ny, :]
                    row.append((mid + mid) + (F[k, t, x, 1 : 1 + ny, :] + F[k, t, x, 3 : 3 + ny, :]))
                s.append(jnp.concatenate(row, axis=1))
            s = banded(jnp.concatenate(s, axis=0))
            for k in range(12):
                for t in range(nt):
                    G[k, t, x] = s[(k - k0) * ny : (k - k0 + 1) * ny, 128 * t : 128 * t + 128]
        return 0

    has_lo = jnp.where(iy > 0, 0.125, 0.0)
    has_hi = jnp.where(iy < NY - 1, 0.125, 0.0)
    rows8 = lax.broadcasted_iota(jnp.int32, (8, 128), 0)

    def row_scale(r):
        idx = rows8 + r
        return jnp.where(idx < 2, has_lo, jnp.where(idx < ny + 2, 0.125, has_hi))

    def hat_plane(x, _):
        inside = jnp.where((x == 1) & (ix == 0), 0.0, jnp.where((x == nx + 2) & (ix == NX - 1), 0.0, 1.0))
        for r in starts:
            scale = row_scale(r) * inside
            for c in range(3):
                s = []
                for t in range(nt):
                    mid = Gv[c, t, x, r : r + 8, :]
                    s.append((mid + mid) + (Gv[c, t, x - 1, r : r + 8, :] + Gv[c, t, x + 1, r : r + 8, :]))
                s = zsmooth(s)
                for t in range(nt):
                    H[c, t, x, r : r + 8, :] = s[t] * scale
        return 0

    keep = [None] * nt
    keep[0] = lane8 >= 2
    keep[nt - 1] = (lane8 < 126) if nt > 1 else (lane8 >= 2) & (lane8 < 126)

    def line_plane(x, sums):
        out = []
        for b, r in enumerate(range(0, ny, 8)):
            here = slice(r + 2, r + 10)
            filtered = []
            for k in range(12):
                s = []
                for t in range(nt):
                    mid = G[k, t, x, r : r + 8, :]
                    s.append((mid + mid) + (G[k, t, x - 1, r : r + 8, :] + G[k, t, x + 1, r : r + 8, :]))
                filtered.append(s)
            hat, d = [], [[[None] * 3 for _ in range(3)] for _ in range(nt)]
            m = [[V[3 + c, t, x, here, :] for c in range(3)] for t in range(nt)]
            for i in range(3):
                mid = [H[i, t, x, here, :] for t in range(nt)]
                hat.append(mid)
                hi, lo = zup(mid), zdown(mid)
                for t in range(nt):
                    d[t][i][0] = m[t][0] * (H[i, t, x + 1, here, :] - H[i, t, x - 1, here, :])
                    d[t][i][1] = m[t][1] * (H[i, t, x, r + 3 : r + 11, :] - H[i, t, x, r + 1 : r + 9, :])
                    d[t][i][2] = m[t][2] * (hi[t] - lo[t])
            num = den = 0.0
            for t in range(nt):
                n, e = model_sums([filtered[k][t] for k in range(6)], [filtered[6 + k][t] for k in range(6)], [h[t] for h in hat], d[t], Q[t, x, here, :])
                if keep[t] is not None:
                    n, e = jnp.where(keep[t], n, 0.0), jnp.where(keep[t], e, 0.0)
                num, den = num + n, den + e
            num = jnp.sum(num, axis=1, keepdims=True)
            den = jnp.sum(den, axis=1, keepdims=True)
            acc = jnp.where(lane8 == G6 * x + 2, num, sums[b])
            out.append(jnp.where(lane8 == G6 * x + 4, den, acc))
        return tuple(out)

    def land_chunk(c):
        for n, (dx, dy) in enumerate(plane_offsets):
            if dx == 0:
                def arrive(n=n):
                    for cp in plane_copies(n, c):
                        cp.wait_recv()
                when(exists(0, -dy), arrive)

    def step(i, sums, smooth=True, hat=True, line=True):
        if line:
            sums = line_plane(i - 4, sums)
        if hat:
            hat_plane(i - 2, 0)
        if smooth:
            smooth_plane(i - 1, 0)
        field_plane(i, 0)
        return sums

    sums = tuple(jnp.zeros((8, 128), jnp.float32) for _ in range(0, ny, 8))
    for c in range(chunks):
        land_chunk(c)
        lo = 3 if c == 0 else chunk * c + 1
        hi = chunk * (c + 1)
        if c == 0:
            velocity_plane(2, 0)
            step(3, sums, False, False, False)
            lax.fori_loop(4, hi + 1, lambda i, q: step(i, q, True, False, False), ())
        elif c == 1:
            lax.fori_loop(lo, min(hi + 1, 8), lambda i, q: step(i, q, True, True, False), ())
            sums = lax.fori_loop(8, hi + 1, step, sums)
        else:
            sums = lax.fori_loop(lo, hi + 1, step, sums)
    velocity_plane(nx + 1, 0)
    smooth_plane(nx, 0)
    hat_plane(nx - 1, 0)
    sums = line_plane(nx - 3, sums)
    hat_plane(nx, 0)
    sums = line_plane(nx - 2, sums)
    sums = line_plane(nx - 1, sums)
    land(lambda d: d[0] != 0 and d[2] == 0)

    def edges(per_side):
        return lambda i: jnp.where(i < len(per_side), per_side[0] + i, nx + 3 - per_side[-1] + i - len(per_side))
    near, inner_planes = edges([1, 2]), edges([2, 3])
    lax.fori_loop(0, 4, lambda i, c: field_plane(near(i), c), 0, unroll=4)
    lax.fori_loop(0, 2, lambda i, c: velocity_plane(i * (nx + 3), c), 0, unroll=2)
    lax.fori_loop(0, 4, lambda i, c: smooth_plane(near(i), c), 0, unroll=4)
    lax.fori_loop(0, 4, lambda i, c: hat_plane(near(i), c), 0, unroll=4)
    sums = lax.fori_loop(0, 4, lambda i, c: line_plane(inner_planes(i), c), sums, unroll=4)
    land(lambda d: d[2] != 0)

    yr = ny + 8
    lane_r = lax.broadcasted_iota(jnp.int32, (yr, 128), 1)
    group_r = (lane_r * 43) >> 8
    inner_r = lane_r - G6 * group_r
    rows_r = lax.broadcasted_iota(jnp.int32, (yr, 128), 0)
    outside = ((group_r == 1) & (ix == 0)) | ((group_r == nx + 2) & (ix == NX - 1))
    outside = outside | ((rows_r < 2) & (iy == 0)) | ((rows_r >= ny + 2) & (iy == NY - 1))
    scale_r = jnp.where(outside, 0.0, 0.125)
    enum, eden = 0.0, 0.0
    fixes = []
    for s in range(2):
        mixed = []
        for k in range(2):
            far = jnp.where(lane_r < 2 * G6, lroll(R[1 - s, 0, k], -G6 * nx), R[1 - s, 1, k])
            mixed.append(jnp.where(lane_r >= G6 * (nx + 2), lroll(R[1 - s, 2, k], G6 * nx), far))
        fields = []
        for f in range(6):
            own = TE[s, f]
            for p in (0, 1, nx + 2, nx + 3):
                if f >= 3 and p in (0, nx + 3):
                    continue
                tile = V[f, 0 if s == 0 else nt - 1, p]
                own = jnp.where(group_r == p, lroll(tile, G6 * p - (0 if s == 0 else 122)), own)
            c = f % 3
            if s == 0:
                fields.append(jnp.where(inner_r < 2, lroll(mixed[f // 3], -2 * c), lroll(own, 2)))
            else:
                fields.append(jnp.where(inner_r >= 4, lroll(mixed[f // 3], 4 - 2 * c), lroll(own, -2)))
        u, m = fields[0:3], fields[3:6]
        for f in range(6):
            E[s, f] = fields[f]
        def shift(a, n):
            return lroll(a, -n)
        d = [[None] * 3 for _ in range(3)]
        for i in range(3):
            d[i][0] = m[0] * (shift(u[i], G6) - shift(u[i], -G6))
            d[i][1] = m[1] * (pltpu.roll(u[i], yr - 1, 0) - pltpu.roll(u[i], 1, 0))
            d[i][2] = m[2] * (shift(u[i], 1) - shift(u[i], -1))
        f, square = tensor(d)
        mag = root(0.5 * square)
        dq = jnp.exp2((-2.0 / 3.0) * jnp.log2(m[0] * m[1] * m[2]))
        EF[s, 15] = dq
        EF[s, 16] = dq * mag
        for c in range(3):
            EF[s, 12 + c] = u[c]
        for k, (a, b) in enumerate(pairs):
            EF[s, k] = u[a] * u[b]
            EF[s, 6 + k] = mag * f[k]
        def lanes_smooth(a):
            b = (a + a) + (shift(a, G6) + shift(a, -G6))
            return (b + b) + (shift(b, 1) + shift(b, -1))
        for c in range(3):
            y = (u[c] + u[c]) + (pltpu.roll(u[c], yr - 1, 0) + pltpu.roll(u[c], 1, 0))
            EG[s, c] = lanes_smooth(y) * scale_r
        own = slice(2, 2 + ny)
        filtered = []
        for k in range(12):
            mid = EF[s, k, own, :]
            filtered.append(lanes_smooth((mid + mid) + (EF[s, k, 1 : 1 + ny, :] + EF[s, k, 3 : 3 + ny, :])))
        hat, dh = [], [[None] * 3 for _ in range(3)]
        me = [E[s, 3 + c, own, :] for c in range(3)]
        for i in range(3):
            mid = EG[s, i, own, :]
            hat.append(mid)
            dh[i][0] = me[0] * (shift(mid, G6) - shift(mid, -G6))
            dh[i][1] = me[1] * (EG[s, i, 3 : 3 + ny, :] - EG[s, i, 1 : 1 + ny, :])
            dh[i][2] = me[2] * (shift(mid, 1) - shift(mid, -1))
        n, e = model_sums(filtered[0:6], filtered[6:12], hat, dh, EF[s, 15, own, :])
        enum, eden = enum + n, eden + e
    enum = enum + lroll(enum, -1)
    eden = lroll(eden + lroll(eden, -1), 2)
    used = (group >= 2) & (group < nx + 2)
    extra = jnp.where(used & (inner == 2), enum, jnp.where(used & (inner == 4), eden, 0.0))
    LS[iz] = jnp.concatenate(sums, axis=0) + extra

    def line_copy(o):
        return pltpu.make_async_remote_copy(
            src_ref=LS.at[iz], dst_ref=LS.at[iz], send_sem=lsend.at[o - 1], recv_sem=lrecv.at[o - 1],
            device_id=(ix, iy, lax.rem(iz + o, NZ)), device_id_type=MESH)
    def line_landing(o):
        src = lax.rem(iz - o + NZ, NZ)
        return pltpu.make_async_remote_copy(
            src_ref=LS.at[src], dst_ref=LS.at[src], send_sem=lsend.at[o - 1], recv_sem=lrecv.at[o - 1],
            device_id=(ix, iy, lax.rem(iz + o, NZ)), device_id_type=MESH)
    for o in range(1, NZ):
        line_copy(o).start()

    lo_fix, hi_fix = EF[0, 16, 2 : 2 + ny, :], EF[1, 16, 2 : 2 + ny, :]
    for x in range(nx):
        p = x + 2
        for t in range(nt):
            tile = M[t, p, 2 : 2 + ny, :]
            if t == 0:
                tile = jnp.where(lane == 0, lroll(lo_fix, -(G6 * p + 2)), tile)
            if t == nt - 1:
                tile = jnp.where(lane == 127, lroll(hi_fix, 127 - (G6 * p + 3)), tile)
            D[x, :, 128 * t : 128 * t + 128] = tile
    save = pltpu.make_async_copy(D, d_out, sem_in.at[2 * nt])
    save.start()

    for o in range(1, NZ):
        line_landing(o).wait_recv()
    total = LS[0]
    for o in range(1, NZ):
        total = total + LS[o]
    unit = 4096.0 * nz * NZ
    coef = (total / unit) / (lroll(total, -2) / unit + eps_line)
    masked = jnp.where(used & (inner == 2), coef, -jnp.inf)
    here_max = masked[0:8]
    for r in range(8, ny, 8):
        here_max = jnp.maximum(here_max, masked[r : r + 8])
    me = ix * NY + iy
    PS[me] = here_max
    def peak_copy(j, a, b, landing):
        tx, ty = lax.rem(ix + a, NX), lax.rem(iy + b, NY)
        slot = me
        if landing:
            slot = lax.rem(ix - a + NX, NX) * NY + lax.rem(iy - b + NY, NY)
        return pltpu.make_async_remote_copy(
            src_ref=PS.at[slot], dst_ref=PS.at[slot], send_sem=psend.at[j], recv_sem=precv.at[j],
            device_id=(tx, ty, iz), device_id_type=MESH)
    for j, (a, b) in enumerate(plane_peers):
        peak_copy(j, a, b, False).start()
    for o in range(1, NZ):
        line_copy(o).wait_send()
    for d, make in everything:
        def left(make=make):
            for c in make():
                c.wait_send()
        when(exists(d[0], d[1]), left)
    for j, (a, b) in enumerate(plane_peers):
        peak_copy(j, a, b, True).wait_recv()
    peak = PS[0]
    for j in range(1, NX * NY):
        peak = jnp.maximum(peak, PS[j])
    coef_out[...] = jnp.minimum(coef, 0.5 * jnp.max(peak, axis=(0, 1), keepdims=True))
    save.wait()
    for j, (a, b) in enumerate(plane_peers):
        peak_copy(j, a, b, False).wait_send()


def scale_kernel(D, coef, visc, coef_out):
    nx, ny = visc.shape[:2]
    lane = lax.broadcasted_iota(jnp.int32, (ny, 128), 1)
    table = coef[...]
    turned = table.T
    for x in range(nx):
        at = G6 * (x + 2) + 2
        column = jnp.sum(jnp.where(lane == at, table, 0.0), axis=1, keepdims=True)
        visc[x] = D[x] * column
        coef_out[x : x + 1, :] = turned[at : at + 1, :]


def per_device(sizes, velocity, metric):
    nx, ny, nz = velocity.shape[1:]
    NX, NY, NZ = sizes
    assert nz % 128 == 0 and ny % 8 == 0 and G6 * (nx + 4) <= 128 and nx >= 6
    nt, px, yr = nz // 128, nx + 4, ny + 8
    f32 = jnp.float32
    copies = len(span_offsets) + (2 * chunks + 1) * len(plane_offsets)
    dmag, coef = pl.pallas_call(
        functools.partial(kernel, sizes),
        out_shape=(jax.ShapeDtypeStruct((nx, ny, nz), f32), jax.ShapeDtypeStruct((ny, 128), f32)),
        in_specs=[pl.BlockSpec(memory_space=pltpu.HBM)] * 2,
        out_specs=(pl.BlockSpec(memory_space=pltpu.HBM), pl.BlockSpec(memory_space=pltpu.VMEM)),
        scratch_shapes=[
            pltpu.VMEM((6, nt, px, yr, 128), f32),
            pltpu.VMEM((3, nt, px, yr, 128), f32),
            pltpu.VMEM((12, nt, px, ny, 128), f32),
            pltpu.VMEM((3, nt, px, yr, 128), f32),
            pltpu.VMEM((nt, px, yr, 128), f32),
            pltpu.VMEM((nt, px, yr, 128), f32),
            pltpu.VMEM((12, nt, px, yr, 128), f32),
            pltpu.VMEM((2, 6, yr, 128), f32),
            pltpu.VMEM((2, 6, yr, 128), f32),
            pltpu.VMEM((2, 17, yr, 128), f32),
            pltpu.VMEM((2, 3, yr, 128), f32),
            pltpu.VMEM((2, 2, ny, 128), f32),
            pltpu.VMEM((2, 3, 2, yr, 128), f32),
            pltpu.VMEM((NZ, ny, 128), f32),
            pltpu.VMEM((NX * NY, 8, 128), f32),
            pltpu.VMEM((nx, ny, nz), f32),
            pltpu.VMEM((nz, nz), jnp.bfloat16),
            pltpu.SemaphoreType.DMA((2 * nt + 1,)),
            pltpu.SemaphoreType.DMA((copies,)),
            pltpu.SemaphoreType.DMA((copies,)),
            pltpu.SemaphoreType.DMA((NZ,)),
            pltpu.SemaphoreType.DMA((NZ,)),
            pltpu.SemaphoreType.DMA((NX * NY,)),
            pltpu.SemaphoreType.DMA((NX * NY,)),
        ],
        compiler_params=pltpu.CompilerParams(collective_id=0, has_side_effects=True, vmem_limit_bytes=67043328 - 600 * 1024),
    )(velocity, metric)
    return pl.pallas_call(
        scale_kernel,
        out_shape=(jax.ShapeDtypeStruct((nx, ny, nz), f32), jax.ShapeDtypeStruct((nx, ny), f32)),
        in_specs=[pl.BlockSpec(memory_space=pltpu.VMEM)] * 2,
        out_specs=(pl.BlockSpec(memory_space=pltpu.VMEM),) * 2,
        compiler_params=pltpu.CompilerParams(vmem_limit_bytes=4 * 1024 * 1024),
    )(dmag, coef)


def solution(mesh):
    sizes = (mesh.shape["gx"], mesh.shape["gy"], mesh.shape["gz"])
    return jax.shard_map(
        functools.partial(per_device, sizes),
        mesh=mesh,
        in_specs=(P(None, "gx", "gy", "gz"), P(None, "gx", "gy", "gz")),
        out_specs=(P("gx", "gy", "gz"), P("gx", "gy")),
        check_vma=False,
    )
```

```python
import functools

import jax
import jax.numpy as jnp
from jax import lax
from jax.experimental import pallas as pl
from jax.experimental.pallas import tpu as pltpu
from jax.sharding import PartitionSpec as P

MESH = pl.DeviceIdType.MESH
pairs = ((0, 0), (1, 1), (2, 2), (0, 1), (0, 2), (1, 2))
eps_line = 1e-06
smallest = 1.1754944e-38
plane_offsets = [(dx, dy) for dx in (0, 1, -1) for dy in (0, 1, -1) if (dx, dy) != (0, 0)]
span_offsets = [(dx, dy, dz) for dz in (1, -1) for dx in (0, 1, -1) for dy in (0, 1, -1)]
chunks = 4
G6 = 6


def root(s):
    return s * lax.rsqrt(jnp.maximum(s, smallest))


def tensor(d):
    f = [d[a][b] if a == b else d[a][b] + d[b][a] for a, b in pairs]
    square = (f[0] * f[0] + f[1] * f[1] + f[2] * f[2]) + 0.5 * (f[3] * f[3] + f[4] * f[4] + f[5] * f[5])
    return f, square


def model_sums(vv, ms, hat, dh, dq):
    f, square = tensor(dh)
    mh = root(8.0 * square)
    num = den = off = None
    for k, (a, b) in enumerate(pairs):
        leonard = vv[k] - hat[a] * hat[b]
        model = ms[k] - mh * f[k]
        n, m2 = leonard * model, model * model
        num = n if num is None else num + n
        if a == b:
            den = m2 if den is None else den + m2
        else:
            off = m2 if off is None else off + m2
    return num * dq, (den + 0.5 * off) * (dq * dq)


def kernel(sizes, vel, met, D, coef_out, V, Gv, G, H, Q, M, F, TE, E, EF, EG, PK, R, LS, PS, W, sem_in, send, recv, lsend, lrecv, psend, precv):
    NX, NY, NZ = sizes
    nx, ny, nz = vel.shape[1:]
    nt = nz // 128
    px = nx + 4
    starts = list(range(1, ny - 6, 8)) + [ny - 5]
    ix, iy, iz = lax.axis_index("gx"), lax.axis_index("gy"), lax.axis_index("gz")

    loads = []
    for k, src in enumerate((vel, met)):
        for t in range(nt):
            loads.append(pltpu.make_async_copy(
                src.at[:, :, :, 128 * t : 128 * t + 128],
                V.at[3 * k : 3 * k + 3, t, 2 : 2 + nx, 2 : 2 + ny, :],
                sem_in.at[k * nt + t]))
    for c in loads:
        c.start()

    def there(delta, i, n):
        return None if delta == 0 else (i + delta >= 0) & (i + delta < n)

    def exists(dx, dy):
        a, b = there(dx, ix, NX), there(dy, iy, NY)
        if a is None:
            return b
        return a if b is None else a & b

    def when(cond, fn):
        if cond is None:
            fn()
        else:
            pl.when(cond)(fn)

    def dev(d):
        return (ix + d[0], iy + d[1], lax.rem(iz + d[2] + NZ, NZ))

    barrier = pltpu.get_barrier_semaphore()
    expected = jnp.int32(0)
    for d in span_offsets + [(dx, dy, 0) for dx, dy in plane_offsets]:
        ok = exists(d[0], d[1])
        def sig(d=d):
            pl.semaphore_signal(barrier, inc=1, device_id=dev(d), device_id_type=MESH)
        when(ok, sig)
        expected = expected + (1 if ok is None else ok.astype(jnp.int32))
    for o in range(1, NZ):
        pl.semaphore_signal(barrier, inc=1, device_id=(ix, iy, lax.rem(iz + o, NZ)), device_id_type=MESH)
    plane_peers = [(a, b) for a in range(NX) for b in range(NY) if (a, b) != (0, 0)]
    for a, b in plane_peers:
        pl.semaphore_signal(barrier, inc=1, device_id=(lax.rem(ix + a, NX), lax.rem(iy + b, NY), iz), device_id_type=MESH)
    expected = expected + (NZ - 1 + len(plane_peers))

    z2 = jnp.zeros((2, 128), jnp.float32)
    for dx, p0 in ((-1, 0), (1, nx + 2)):
        def clear_planes(dx=dx, p0=p0):
            for f in range(6):
                for t in range(nt):
                    for p in (p0, p0 + 1):
                        V[f, t, p] = jnp.zeros((ny + 8, 128), jnp.float32)
            for s in range(2):
                for k in range(2):
                    R[s, dx + 1, k] = jnp.zeros((ny + 8, 128), jnp.float32)
        pl.when(jnp.logical_not(there(dx, ix, NX)))(clear_planes)
    for dy, r0 in ((-1, 0), (1, ny + 2)):
        def clear_rows(r0=r0):
            def body(p, _):
                for f in range(6):
                    for t in range(nt):
                        V[f, t, p, r0 : r0 + 2, :] = z2
                return 0
            lax.fori_loop(0, px, body, 0)
            for s in range(2):
                for f in range(6):
                    TE[s, f, r0 : r0 + 2, :] = z2
                for dxi in range(3):
                    for k in range(2):
                        R[s, dxi, k, r0 : r0 + 2, :] = z2
        pl.when(jnp.logical_not(there(dy, iy, NY)))(clear_rows)

    for c in loads:
        c.wait()

    lane = lax.broadcasted_iota(jnp.int32, (ny, 128), 1)
    group = (lane * 43) >> 8
    inner = lane - G6 * group
    lane8, group8, inner8 = lane[0:8], group[0:8], inner[0:8]

    def lroll(a, s):
        s = s % 128
        return pltpu.roll(a, s, 1) if s else a

    pl.semaphore_wait(barrier, expected)

    def span_x(dx, deep):
        if dx == 0:
            return (2, 2, nx)
        if dx == 1:
            return (nx, 0, 2) if deep else (nx + 1, 1, 1)
        return (2, nx + 2, 2) if deep else (2, nx + 2, 1)

    def span_y(dy, deep):
        if dy == 0:
            return (2, 2, ny)
        if dy == 1:
            return (ny, 0, 2) if deep else (ny + 1, 1, 1)
        return (2, ny + 2, 2) if deep else (2, ny + 2, 1)

    def remote(src, dst, j, d):
        return pltpu.make_async_remote_copy(src_ref=src, dst_ref=dst, send_sem=send.at[j], recv_sem=recv.at[j], device_id=dev(d), device_id_type=MESH)

    def span_copy(n):
        dx, dy, dz = d = span_offsets[n]
        s = 1 if dz == 1 else 0
        ys, yd, yn = span_y(dy, True)
        return remote(PK.at[s, :, ys - 2 : ys - 2 + yn, :], R.at[s, 1 - dx, :, yd : yd + yn, :], n, d)

    chunk = nx // chunks

    def plane_copies(n, part=None):
        dx, dy = plane_offsets[n]
        d = (dx, dy, 0)
        base = len(span_offsets) + (2 * chunks + 1) * n
        out = []
        for c in range(chunks if dx == 0 else 1):
            if part is not None and c != part:
                continue
            for k in range(2):
                xs, xd, xn = span_x(dx, k == 0)
                if dx == 0:
                    xs, xd, xn = 2 + c * chunk, 2 + c * chunk, chunk
                ys, yd, yn = span_y(dy, k == 0)
                f0 = 3 * k
                out.append(remote(V.at[f0 : f0 + 3, :, xs : xs + xn, ys : ys + yn, :], V.at[f0 : f0 + 3, :, xd : xd + xn, yd : yd + yn, :], base + 2 * c + k, d))
        return out

    def edge_rows(n):
        dx, dy = plane_offsets[n]
        ys, yd, yn = span_y(dy, True)
        return remote(TE.at[:, :, ys : ys + yn, :], TE.at[:, :, yd : yd + yn, :], len(span_offsets) + (2 * chunks + 1) * n + 2 * chunks, (dx, dy, 0))

    everything = [(d, (lambda n=n: [span_copy(n)])) for n, d in enumerate(span_offsets)]
    everything += [((dx, dy, 0), (lambda n=n: plane_copies(n))) for n, (dx, dy) in enumerate(plane_offsets)]
    def send_all(wanted):
        for d, make in everything:
            if wanted(d):
                def go(make=make):
                    for c in make():
                        c.start()
                when(exists(d[0], d[1]), go)

    send_all(lambda d: d[2] == 0 and d[0] == 0)
    send_all(lambda d: d[2] == 0 and d[0] != 0)
    for f in range(6):
        for s in range(2):
            acc = jnp.zeros((ny, 128), jnp.float32)
            for p in range(2, 2 + nx):
                tile = V[f, 0 if s == 0 else nt - 1, p, 2 : 2 + ny, :]
                acc = jnp.where(group == p, lroll(tile, G6 * p - (0 if s == 0 else 122)), acc)
            TE[s, f, 2 : 2 + ny, :] = acc
    for s in range(2):
        for k in range(2):
            parts = [lroll(TE[s, 3 * k + c, 2 : 2 + ny, :], 2 * c - (0 if s == 0 else 4)) for c in range(3)]
            PK[s, k] = jnp.where(inner < 2, parts[0], jnp.where(inner < 4, parts[1], parts[2]))

    for n, (dx, dy) in enumerate(plane_offsets):
        if dx == 0:
            when(exists(dx, dy), lambda n=n: edge_rows(n).start())
    send_all(lambda d: d[2] != 0)
    def land(wanted):
        for d, make in everything:
            if wanted(d):
                def arrive(make=make):
                    for c in make():
                        c.wait_recv()
                when(exists(-d[0], -d[1]), arrive)

    first, last = lane8 == 0, lane8 == 127

    def zup(a):
        r = [pltpu.roll(v, 127, 1) for v in a]
        return [jnp.where(last, r[(t + 1) % nt], r[t]) for t in range(nt)]

    def zdown(a):
        r = [pltpu.roll(v, 1, 1) for v in a]
        return [jnp.where(first, r[t - 1], r[t]) for t in range(nt)]

    def zsmooth(a):
        return [(v + v) + (w + q) for v, w, q in zip(a, zup(a), zdown(a))]

    def field_plane(x, _):
        for r in starts:
            here = slice(r, r + 8)
            m = [[V[3 + c, t, x, here, :] for c in range(3)] for t in range(nt)]
            u, d = [], [[[None] * 3 for _ in range(3)] for _ in range(nt)]
            for i in range(3):
                mid = [V[i, t, x, here, :] for t in range(nt)]
                u.append(mid)
                hi, lo = zup(mid), zdown(mid)
                for t in range(nt):
                    above, below = V[i, t, x, r + 1 : r + 9, :], V[i, t, x, r - 1 : r + 7, :]
                    Gv[i, t, x, here, :] = (mid[t] + mid[t]) + (above + below)
                    d[t][i][0] = m[t][0] * (V[i, t, x + 1, here, :] - V[i, t, x - 1, here, :])
                    d[t][i][1] = m[t][1] * (above - below)
                    d[t][i][2] = m[t][2] * (hi[t] - lo[t])
            for t in range(nt):
                f, square = tensor(d[t])
                mag = root(0.5 * square)
                dq = jnp.exp2((-2.0 / 3.0) * jnp.log2(m[t][0] * m[t][1] * m[t][2]))
                Q[t, x, here, :] = dq
                M[t, x, here, :] = dq * mag
                for k, (a, b) in enumerate(pairs):
                    F[k, t, x, here, :] = u[a][t] * u[b][t]
                    F[6 + k, t, x, here, :] = mag * f[k]
        return 0

    def velocity_plane(x, _):
        for c in range(3):
            for t in range(nt):
                for r in starts:
                    mid = V[c, t, x, r : r + 8, :]
                    Gv[c, t, x, r : r + 8, :] = (mid + mid) + (V[c, t, x, r - 1 : r + 7, :] + V[c, t, x, r + 1 : r + 9, :])
        return 0

    zi = lax.broadcasted_iota(jnp.int32, (nz, nz), 0)
    zj = lax.broadcasted_iota(jnp.int32, (nz, nz), 1)
    gap = jnp.abs(zi - zj)
    W[...] = jnp.where(gap == 0, 2.0, jnp.where((gap == 1) | (gap == nz - 1), 1.0, 0.0)).astype(jnp.bfloat16)

    def banded(a):
        w = W[...]
        hi = a.astype(jnp.bfloat16)
        rest = a - hi.astype(jnp.float32)
        mid = rest.astype(jnp.bfloat16)
        low = (rest - mid.astype(jnp.float32)).astype(jnp.bfloat16)
        n = a.shape[0]
        out = jnp.dot(jnp.concatenate([hi, mid, low], axis=0), w, preferred_element_type=jnp.float32)
        return out[0:n] + (out[n : 2 * n] + out[2 * n :])

    def smooth_plane(x, _):
        for k0 in (0,):
            s = []
            for k in range(12):
                row = []
                for t in range(nt):
                    mid = F[k, t, x, 2 : 2 + ny, :]
                    row.append((mid + mid) + (F[k, t, x, 1 : 1 + ny, :] + F[k, t, x, 3 : 3 + ny, :]))
                s.append(jnp.concatenate(row, axis=1))
            s = banded(jnp.concatenate(s, axis=0))
            for k in range(12):
                for t in range(nt):
                    G[k, t, x] = s[(k - k0) * ny : (k - k0 + 1) * ny, 128 * t : 128 * t + 128]
        return 0

    has_lo = jnp.where(iy > 0, 0.125, 0.0)
    has_hi = jnp.where(iy < NY - 1, 0.125, 0.0)
    rows8 = lax.broadcasted_iota(jnp.int32, (8, 128), 0)

    def row_scale(r):
        idx = rows8 + r
        return jnp.where(idx < 2, has_lo, jnp.where(idx < ny + 2, 0.125, has_hi))

    def hat_plane(x, _):
        inside = jnp.where((x == 1) & (ix == 0), 0.0, jnp.where((x == nx + 2) & (ix == NX - 1), 0.0, 1.0))
        for r in starts:
            scale = row_scale(r) * inside
            for c in range(3):
                s = []
                for t in range(nt):
                    mid = Gv[c, t, x, r : r + 8, :]
                    s.append((mid + mid) + (Gv[c, t, x - 1, r : r + 8, :] + Gv[c, t, x + 1, r : r + 8, :]))
                s = zsmooth(s)
                for t in range(nt):
                    H[c, t, x, r : r + 8, :] = s[t] * scale
        return 0

    keep = [None] * nt
    keep[0] = lane8 >= 2
    keep[nt - 1] = (lane8 < 126) if nt > 1 else (lane8 >= 2) & (lane8 < 126)

    def line_plane(x, sums):
        out = []
        for b, r in enumerate(range(0, ny, 8)):
            here = slice(r + 2, r + 10)
            filtered = []
            for k in range(12):
                s = []
                for t in range(nt):
                    mid = G[k, t, x, r : r + 8, :]
                    s.append((mid + mid) + (G[k, t, x - 1, r : r + 8, :] + G[k, t, x + 1, r : r + 8, :]))
                filtered.append(s)
            hat, d = [], [[[None] * 3 for _ in range(3)] for _ in range(nt)]
            m = [[V[3 + c, t, x, here, :] for c in range(3)] for t in range(nt)]
            for i in range(3):
                mid = [H[i, t, x, here, :] for t in range(nt)]
                hat.append(mid)
                hi, lo = zup(mid), zdown(mid)
                for t in range(nt):
                    d[t][i][0] = m[t][0] * (H[i, t, x + 1, here, :] - H[i, t, x - 1, here, :])
                    d[t][i][1] = m[t][1] * (H[i, t, x, r + 3 : r + 11, :] - H[i, t, x, r + 1 : r + 9, :])
                    d[t][i][2] = m[t][2] * (hi[t] - lo[t])
            num = den = 0.0
            for t in range(nt):
                n, e = model_sums([filtered[k][t] for k in range(6)], [filtered[6 + k][t] for k in range(6)], [h[t] for h in hat], d[t], Q[t, x, here, :])
                if keep[t] is not None:
                    n, e = jnp.where(keep[t], n, 0.0), jnp.where(keep[t], e, 0.0)
                num, den = num + n, den + e
            num = jnp.sum(num, axis=1, keepdims=True)
            den = jnp.sum(den, axis=1, keepdims=True)
            acc = jnp.where(lane8 == G6 * x + 2, num, sums[b])
            out.append(jnp.where(lane8 == G6 * x + 4, den, acc))
        return tuple(out)

    def land_chunk(c):
        for n, (dx, dy) in enumerate(plane_offsets):
            if dx == 0:
                def arrive(n=n):
                    for cp in plane_copies(n, c):
                        cp.wait_recv()
                when(exists(0, -dy), arrive)

    def step(i, sums, smooth=True, hat=True, line=True):
        if line:
            sums = line_plane(i - 4, sums)
        if hat:
            hat_plane(i - 2, 0)
        if smooth:
            smooth_plane(i - 1, 0)
        field_plane(i, 0)
        return sums

    sums = tuple(jnp.zeros((8, 128), jnp.float32) for _ in range(0, ny, 8))
    for c in range(chunks):
        land_chunk(c)
        lo = 3 if c == 0 else chunk * c + 1
        hi = chunk * (c + 1)
        if c == 0:
            velocity_plane(2, 0)
            step(3, sums, False, False, False)
            lax.fori_loop(4, hi + 1, lambda i, q: step(i, q, True, False, False), ())
        elif c == 1:
            lax.fori_loop(lo, min(hi + 1, 8), lambda i, q: step(i, q, True, True, False), ())
            sums = lax.fori_loop(8, hi + 1, step, sums)
        else:
            sums = lax.fori_loop(lo, hi + 1, step, sums)
    land(lambda d: d[0] != 0 and d[2] == 0)

    land(lambda d: d[2] != 0)
    for n, (dx, dy) in enumerate(plane_offsets):
        if dx == 0:
            when(exists(dx, -dy), lambda n=n: edge_rows(n).wait_recv())
    def edges(per_side):
        return lambda i: jnp.where(i < len(per_side), per_side[0] + i, nx + 3 - per_side[-1] + i - len(per_side))
    near, inner_planes = edges([1, 2]), edges([2, 3])
    velocity_plane(nx + 1, 0)
    smooth_plane(nx, 0)
    hat_plane(nx - 1, 0)
    sums = line_plane(nx - 3, sums)
    hat_plane(nx, 0)
    sums = line_plane(nx - 2, sums)
    sums = line_plane(nx - 1, sums)
    lax.fori_loop(0, 4, lambda i, c: field_plane(near(i), c), 0, unroll=4)
    lax.fori_loop(0, 2, lambda i, c: velocity_plane(i * (nx + 3), c), 0, unroll=2)
    lax.fori_loop(0, 4, lambda i, c: smooth_plane(near(i), c), 0, unroll=4)
    lax.fori_loop(0, 4, lambda i, c: hat_plane(near(i), c), 0, unroll=4)
    sums = lax.fori_loop(0, 4, lambda i, c: line_plane(inner_planes(i), c), sums, unroll=4)

    yr = ny + 8
    lane_r = lax.broadcasted_iota(jnp.int32, (yr, 128), 1)
    group_r = (lane_r * 43) >> 8
    inner_r = lane_r - G6 * group_r
    rows_r = lax.broadcasted_iota(jnp.int32, (yr, 128), 0)
    outside = ((group_r == 1) & (ix == 0)) | ((group_r == nx + 2) & (ix == NX - 1))
    outside = outside | ((rows_r < 2) & (iy == 0)) | ((rows_r >= ny + 2) & (iy == NY - 1))
    scale_r = jnp.where(outside, 0.0, 0.125)
    enum, eden = 0.0, 0.0
    fixes = []
    for s in range(2):
        mixed = []
        for k in range(2):
            far = jnp.where(lane_r < 2 * G6, lroll(R[1 - s, 0, k], -G6 * nx), R[1 - s, 1, k])
            mixed.append(jnp.where(lane_r >= G6 * (nx + 2), lroll(R[1 - s, 2, k], G6 * nx), far))
        fields = []
        for f in range(6):
            own = TE[s, f]
            for p in (0, 1, nx + 2, nx + 3):
                if f >= 3 and p in (0, nx + 3):
                    continue
                tile = V[f, 0 if s == 0 else nt - 1, p]
                own = jnp.where(group_r == p, lroll(tile, G6 * p - (0 if s == 0 else 122)), own)
            c = f % 3
            if s == 0:
                fields.append(jnp.where(inner_r < 2, lroll(mixed[f // 3], -2 * c), lroll(own, 2)))
            else:
                fields.append(jnp.where(inner_r >= 4, lroll(mixed[f // 3], 4 - 2 * c), lroll(own, -2)))
        u, m = fields[0:3], fields[3:6]
        for f in range(6):
            E[s, f] = fields[f]
        def shift(a, n):
            return lroll(a, -n)
        d = [[None] * 3 for _ in range(3)]
        for i in range(3):
            d[i][0] = m[0] * (shift(u[i], G6) - shift(u[i], -G6))
            d[i][1] = m[1] * (pltpu.roll(u[i], yr - 1, 0) - pltpu.roll(u[i], 1, 0))
            d[i][2] = m[2] * (shift(u[i], 1) - shift(u[i], -1))
        f, square = tensor(d)
        mag = root(0.5 * square)
        dq = jnp.exp2((-2.0 / 3.0) * jnp.log2(m[0] * m[1] * m[2]))
        EF[s, 15] = dq
        EF[s, 16] = dq * mag
        for c in range(3):
            EF[s, 12 + c] = u[c]
        for k, (a, b) in enumerate(pairs):
            EF[s, k] = u[a] * u[b]
            EF[s, 6 + k] = mag * f[k]
        def lanes_smooth(a):
            b = (a + a) + (shift(a, G6) + shift(a, -G6))
            return (b + b) + (shift(b, 1) + shift(b, -1))
        for c in range(3):
            y = (u[c] + u[c]) + (pltpu.roll(u[c], yr - 1, 0) + pltpu.roll(u[c], 1, 0))
            EG[s, c] = lanes_smooth(y) * scale_r
        own = slice(2, 2 + ny)
        filtered = []
        for k in range(12):
            mid = EF[s, k, own, :]
            filtered.append(lanes_smooth((mid + mid) + (EF[s, k, 1 : 1 + ny, :] + EF[s, k, 3 : 3 + ny, :])))
        hat, dh = [], [[None] * 3 for _ in range(3)]
        me = [E[s, 3 + c, own, :] for c in range(3)]
        for i in range(3):
            mid = EG[s, i, own, :]
            hat.append(mid)
            dh[i][0] = me[0] * (shift(mid, G6) - shift(mid, -G6))
            dh[i][1] = me[1] * (EG[s, i, 3 : 3 + ny, :] - EG[s, i, 1 : 1 + ny, :])
            dh[i][2] = me[2] * (shift(mid, 1) - shift(mid, -1))
        n, e = model_sums(filtered[0:6], filtered[6:12], hat, dh, EF[s, 15, own, :])
        enum, eden = enum + n, eden + e
    enum = enum + lroll(enum, -1)
    eden = lroll(eden + lroll(eden, -1), 2)
    used = (group >= 2) & (group < nx + 2)
    extra = jnp.where(used & (inner == 2), enum, jnp.where(used & (inner == 4), eden, 0.0))
    LS[iz] = jnp.concatenate(sums, axis=0) + extra

    def line_copy(o):
        return pltpu.make_async_remote_copy(
            src_ref=LS.at[iz], dst_ref=LS.at[iz], send_sem=lsend.at[o - 1], recv_sem=lrecv.at[o - 1],
            device_id=(ix, iy, lax.rem(iz + o, NZ)), device_id_type=MESH)
    def line_landing(o):
        src = lax.rem(iz - o + NZ, NZ)
        return pltpu.make_async_remote_copy(
            src_ref=LS.at[src], dst_ref=LS.at[src], send_sem=lsend.at[o - 1], recv_sem=lrecv.at[o - 1],
            device_id=(ix, iy, lax.rem(iz + o, NZ)), device_id_type=MESH)
    for o in range(1, NZ):
        line_copy(o).start()

    lo_fix, hi_fix = EF[0, 16, 2 : 2 + ny, :], EF[1, 16, 2 : 2 + ny, :]
    for x in range(nx):
        p = x + 2
        for t in range(nt):
            tile = M[t, p, 2 : 2 + ny, :]
            if t == 0:
                tile = jnp.where(lane == 0, lroll(lo_fix, -(G6 * p + 2)), tile)
            if t == nt - 1:
                tile = jnp.where(lane == 127, lroll(hi_fix, 127 - (G6 * p + 3)), tile)
            D[x, :, 128 * t : 128 * t + 128] = tile

    for o in range(1, NZ):
        line_landing(o).wait_recv()
    total = LS[0]
    for o in range(1, NZ):
        total = total + LS[o]
    unit = 4096.0 * nz * NZ
    coef = (total / unit) / (lroll(total, -2) / unit + eps_line)
    masked = jnp.where(used & (inner == 2), coef, -jnp.inf)
    here_max = masked[0:8]
    for r in range(8, ny, 8):
        here_max = jnp.maximum(here_max, masked[r : r + 8])
    me = ix * NY + iy
    PS[me] = here_max
    def peak_copy(j, a, b, landing):
        tx, ty = lax.rem(ix + a, NX), lax.rem(iy + b, NY)
        slot = me
        if landing:
            slot = lax.rem(ix - a + NX, NX) * NY + lax.rem(iy - b + NY, NY)
        return pltpu.make_async_remote_copy(
            src_ref=PS.at[slot], dst_ref=PS.at[slot], send_sem=psend.at[j], recv_sem=precv.at[j],
            device_id=(tx, ty, iz), device_id_type=MESH)
    for j, (a, b) in enumerate(plane_peers):
        peak_copy(j, a, b, False).start()
    for o in range(1, NZ):
        line_copy(o).wait_send()
    for d, make in everything:
        def left(make=make):
            for c in make():
                c.wait_send()
        when(exists(d[0], d[1]), left)
    for n, (dx, dy) in enumerate(plane_offsets):
        if dx == 0:
            when(exists(dx, dy), lambda n=n: edge_rows(n).wait_send())
    for j, (a, b) in enumerate(plane_peers):
        peak_copy(j, a, b, True).wait_recv()
    peak = PS[0]
    for j in range(1, NX * NY):
        peak = jnp.maximum(peak, PS[j])
    coef_out[...] = jnp.minimum(coef, 0.5 * jnp.max(peak, axis=(0, 1), keepdims=True))
    for j, (a, b) in enumerate(plane_peers):
        peak_copy(j, a, b, False).wait_send()


def scale_kernel(D, coef, visc, coef_out):
    nx, ny = visc.shape[:2]
    lane = lax.broadcasted_iota(jnp.int32, (ny, 128), 1)
    table = coef[...]
    turned = table.T
    for x in range(nx):
        at = G6 * (x + 2) + 2
        column = jnp.sum(jnp.where(lane == at, table, 0.0), axis=1, keepdims=True)
        visc[x] = D[x] * column
        coef_out[x : x + 1, :] = turned[at : at + 1, :]


def per_device(sizes, velocity, metric):
    nx, ny, nz = velocity.shape[1:]
    NX, NY, NZ = sizes
    assert nz % 128 == 0 and ny % 8 == 0 and G6 * (nx + 4) <= 128 and nx >= 6
    nt, px, yr = nz // 128, nx + 4, ny + 8
    f32 = jnp.float32
    copies = len(span_offsets) + (2 * chunks + 1) * len(plane_offsets)
    dmag, coef = pl.pallas_call(
        functools.partial(kernel, sizes),
        out_shape=(pltpu.VMEM((nx, ny, nz), f32), pltpu.VMEM((ny, 128), f32)),
        in_specs=[pl.BlockSpec(memory_space=pltpu.HBM)] * 2,
        out_specs=(pl.BlockSpec(memory_space=pltpu.VMEM), pl.BlockSpec(memory_space=pltpu.VMEM)),
        scratch_shapes=[
            pltpu.VMEM((6, nt, px, yr, 128), f32),
            pltpu.VMEM((3, nt, px, yr, 128), f32),
            pltpu.VMEM((12, nt, px, ny, 128), f32),
            pltpu.VMEM((3, nt, px, yr, 128), f32),
            pltpu.VMEM((nt, px, yr, 128), f32),
            pltpu.VMEM((nt, px, yr, 128), f32),
            pltpu.VMEM((12, nt, px, yr, 128), f32),
            pltpu.VMEM((2, 6, yr, 128), f32),
            pltpu.VMEM((2, 6, yr, 128), f32),
            pltpu.VMEM((2, 17, yr, 128), f32),
            pltpu.VMEM((2, 3, yr, 128), f32),
            pltpu.VMEM((2, 2, ny, 128), f32),
            pltpu.VMEM((2, 3, 2, yr, 128), f32),
            pltpu.VMEM((NZ, ny, 128), f32),
            pltpu.VMEM((NX * NY, 8, 128), f32),
            pltpu.VMEM((nz, nz), jnp.bfloat16),
            pltpu.SemaphoreType.DMA((2 * nt + 1,)),
            pltpu.SemaphoreType.DMA((copies,)),
            pltpu.SemaphoreType.DMA((copies,)),
            pltpu.SemaphoreType.DMA((NZ,)),
            pltpu.SemaphoreType.DMA((NZ,)),
            pltpu.SemaphoreType.DMA((NX * NY,)),
            pltpu.SemaphoreType.DMA((NX * NY,)),
        ],
        compiler_params=pltpu.CompilerParams(collective_id=0, has_side_effects=True, vmem_limit_bytes=67043328 - 600 * 1024),
    )(velocity, metric)
    return pl.pallas_call(
        scale_kernel,
        out_shape=(jax.ShapeDtypeStruct((nx, ny, nz), f32), jax.ShapeDtypeStruct((nx, ny), f32)),
        in_specs=[pl.BlockSpec(memory_space=pltpu.VMEM)] * 2,
        out_specs=(pl.BlockSpec(memory_space=pltpu.VMEM),) * 2,
        compiler_params=pltpu.CompilerParams(vmem_limit_bytes=4 * 1024 * 1024),
    )(dmag, coef)


def solution(mesh):
    sizes = (mesh.shape["gx"], mesh.shape["gy"], mesh.shape["gz"])
    return jax.shard_map(
        functools.partial(per_device, sizes),
        mesh=mesh,
        in_specs=(P(None, "gx", "gy", "gz"), P(None, "gx", "gy", "gz")),
        out_specs=(P("gx", "gy", "gz"), P("gx", "gy")),
        check_vma=False,
    )
```

```python
import functools

import jax
import jax.numpy as jnp
from jax import lax
from jax.experimental import pallas as pl
from jax.experimental.pallas import tpu as pltpu
from jax.sharding import PartitionSpec as P

MESH = pl.DeviceIdType.MESH
pairs = ((0, 0), (1, 1), (2, 2), (0, 1), (0, 2), (1, 2))
eps_line = 1e-06
smallest = 1.1754944e-38
plane_offsets = [(dx, dy) for dx in (0, 1, -1) for dy in (0, 1, -1) if (dx, dy) != (0, 0)]
span_offsets = [(dx, dy, dz) for dz in (1, -1) for dx in (0, 1, -1) for dy in (0, 1, -1)]
chunks = 4
G6 = 6


def root(s):
    return s * lax.rsqrt(jnp.maximum(s, smallest))


def tensor(d):
    f = [d[a][b] if a == b else d[a][b] + d[b][a] for a, b in pairs]
    square = (f[0] * f[0] + f[1] * f[1] + f[2] * f[2]) + 0.5 * (f[3] * f[3] + f[4] * f[4] + f[5] * f[5])
    return f, square


def model_sums(vv, ms, hat, dh, dq):
    f, square = tensor(dh)
    mh = root(8.0 * square)
    num = den = off = None
    for k, (a, b) in enumerate(pairs):
        leonard = vv[k] - hat[a] * hat[b]
        model = ms[k] - mh * f[k]
        n, m2 = leonard * model, model * model
        num = n if num is None else num + n
        if a == b:
            den = m2 if den is None else den + m2
        else:
            off = m2 if off is None else off + m2
    return num * dq, (den + 0.5 * off) * (dq * dq)


def kernel(sizes, vel, met, D, coef_out, V, Gv, G, H, Q, M, F, TE, E, EF, EG, PK, R, LS, PS, W, token, sem_in, send, recv, lsend, lrecv, psend, precv):
    NX, NY, NZ = sizes
    nx, ny, nz = vel.shape[1:]
    nt = nz // 128
    px = nx + 4
    starts = list(range(1, ny - 6, 8)) + [ny - 5]
    ix, iy, iz = lax.axis_index("gx"), lax.axis_index("gy"), lax.axis_index("gz")

    loads = []
    for k, src in enumerate((vel, met)):
        for t in range(nt):
            loads.append(pltpu.make_async_copy(
                src.at[:, :, :, 128 * t : 128 * t + 128],
                V.at[3 * k : 3 * k + 3, t, 2 : 2 + nx, 2 : 2 + ny, :],
                sem_in.at[k * nt + t]))
    for c in loads:
        c.start()

    def there(delta, i, n):
        return None if delta == 0 else (i + delta >= 0) & (i + delta < n)

    def exists(dx, dy):
        a, b = there(dx, ix, NX), there(dy, iy, NY)
        if a is None:
            return b
        return a if b is None else a & b

    def when(cond, fn):
        if cond is None:
            fn()
        else:
            pl.when(cond)(fn)

    def dev(d):
        return (ix + d[0], iy + d[1], lax.rem(iz + d[2] + NZ, NZ))

    barrier = pltpu.get_barrier_semaphore()
    expected = jnp.int32(0)
    plane_peers = [(a, b) for a in range(NX) for b in range(NY) if (a, b) != (0, 0)]
    for a, b in plane_peers:
        pl.semaphore_signal(barrier, inc=1, device_id=(lax.rem(ix + a, NX), lax.rem(iy + b, NY), iz), device_id_type=MESH)
    expected = expected + len(plane_peers)
    for dz in (1, -1):
        ok = there(dz, iz, NZ)
        pl.when(ok)(lambda dz=dz: pl.semaphore_signal(barrier, inc=1, device_id=(ix, iy, iz + dz), device_id_type=MESH))
        expected = expected + ok.astype(jnp.int32)

    def tell(dz):
        pl.when(there(dz, iz, NZ))(lambda: pl.semaphore_signal(token.at[(dz + 1) // 2], inc=1, device_id=(ix, iy, iz + dz), device_id_type=MESH))

    def relay(dz):
        def hear():
            pl.semaphore_wait(token.at[(dz + 1) // 2], 1)
            tell(dz)
        pl.when(there(-dz, iz, NZ))(hear)

    z2 = jnp.zeros((2, 128), jnp.float32)
    for dx, p0 in ((-1, 0), (1, nx + 2)):
        def clear_planes(dx=dx, p0=p0):
            for f in range(6):
                for t in range(nt):
                    for p in (p0, p0 + 1):
                        V[f, t, p] = jnp.zeros((ny + 8, 128), jnp.float32)
            for s in range(2):
                for k in range(2):
                    R[s, dx + 1, k] = jnp.zeros((ny + 8, 128), jnp.float32)
        pl.when(jnp.logical_not(there(dx, ix, NX)))(clear_planes)
    for dy, r0 in ((-1, 0), (1, ny + 2)):
        def clear_rows(r0=r0):
            def body(p, _):
                for f in range(6):
                    for t in range(nt):
                        V[f, t, p, r0 : r0 + 2, :] = z2
                return 0
            lax.fori_loop(0, px, body, 0)
            for s in range(2):
                for f in range(6):
                    TE[s, f, r0 : r0 + 2, :] = z2
                for dxi in range(3):
                    for k in range(2):
                        R[s, dxi, k, r0 : r0 + 2, :] = z2
        pl.when(jnp.logical_not(there(dy, iy, NY)))(clear_rows)

    pl.semaphore_wait(barrier, expected)
    for dz in (1, -1):
        pl.when(jnp.logical_not(there(-dz, iz, NZ)))(functools.partial(tell, dz))
    for c in loads:
        c.wait()

    lane = lax.broadcasted_iota(jnp.int32, (ny, 128), 1)
    group = (lane * 43) >> 8
    inner = lane - G6 * group
    lane8, group8, inner8 = lane[0:8], group[0:8], inner[0:8]

    def lroll(a, s):
        s = s % 128
        return pltpu.roll(a, s, 1) if s else a


    def span_x(dx, deep):
        if dx == 0:
            return (2, 2, nx)
        if dx == 1:
            return (nx, 0, 2) if deep else (nx + 1, 1, 1)
        return (2, nx + 2, 2) if deep else (2, nx + 2, 1)

    def span_y(dy, deep):
        if dy == 0:
            return (2, 2, ny)
        if dy == 1:
            return (ny, 0, 2) if deep else (ny + 1, 1, 1)
        return (2, ny + 2, 2) if deep else (2, ny + 2, 1)

    def remote(src, dst, j, d):
        return pltpu.make_async_remote_copy(src_ref=src, dst_ref=dst, send_sem=send.at[j], recv_sem=recv.at[j], device_id=dev(d), device_id_type=MESH)

    def span_copy(n):
        dx, dy, dz = d = span_offsets[n]
        s = 1 if dz == 1 else 0
        ys, yd, yn = span_y(dy, True)
        return remote(PK.at[s, :, ys - 2 : ys - 2 + yn, :], R.at[s, 1 - dx, :, yd : yd + yn, :], n, d)

    chunk = nx // chunks

    def plane_copies(n, part=None):
        dx, dy = plane_offsets[n]
        d = (dx, dy, 0)
        base = len(span_offsets) + (2 * chunks + 1) * n
        out = []
        for c in range(chunks if dx == 0 else 1):
            if part is not None and c != part:
                continue
            for k in range(2):
                xs, xd, xn = span_x(dx, k == 0)
                if dx == 0:
                    xs, xd, xn = 2 + c * chunk, 2 + c * chunk, chunk
                ys, yd, yn = span_y(dy, k == 0)
                f0 = 3 * k
                out.append(remote(V.at[f0 : f0 + 3, :, xs : xs + xn, ys : ys + yn, :], V.at[f0 : f0 + 3, :, xd : xd + xn, yd : yd + yn, :], base + 2 * c + k, d))
        return out

    def edge_rows(n):
        dx, dy = plane_offsets[n]
        ys, yd, yn = span_y(dy, True)
        return remote(TE.at[:, :, ys : ys + yn, :], TE.at[:, :, yd : yd + yn, :], len(span_offsets) + (2 * chunks + 1) * n + 2 * chunks, (dx, dy, 0))

    everything = [(d, (lambda n=n: [span_copy(n)])) for n, d in enumerate(span_offsets)]
    everything += [((dx, dy, 0), (lambda n=n: plane_copies(n))) for n, (dx, dy) in enumerate(plane_offsets)]
    def send_all(wanted):
        for d, make in everything:
            if wanted(d):
                def go(make=make):
                    for c in make():
                        c.start()
                when(exists(d[0], d[1]), go)

    def send_chunk(c):
        for n, (dx, dy) in enumerate(plane_offsets):
            if dx == 0:
                def go(n=n):
                    for cp in plane_copies(n, c):
                        cp.start()
                when(exists(0, dy), go)

    send_chunk(0)
    for f in range(6):
        for s in range(2):
            acc = jnp.zeros((ny, 128), jnp.float32)
            for p in range(2, 2 + nx):
                tile = V[f, 0 if s == 0 else nt - 1, p, 2 : 2 + ny, :]
                acc = jnp.where(group == p, lroll(tile, G6 * p - (0 if s == 0 else 122)), acc)
            TE[s, f, 2 : 2 + ny, :] = acc
    for s in range(2):
        for k in range(2):
            parts = [lroll(TE[s, 3 * k + c, 2 : 2 + ny, :], 2 * c - (0 if s == 0 else 4)) for c in range(3)]
            PK[s, k] = jnp.where(inner < 2, parts[0], jnp.where(inner < 4, parts[1], parts[2]))

    for c in range(1, chunks):
        send_chunk(c)
    for n, (dx, dy) in enumerate(plane_offsets):
        if dx == 0:
            when(exists(dx, dy), lambda n=n: edge_rows(n).start())
    send_all(lambda d: d[2] == 0 and d[0] != 0)
    relay(1)
    relay(-1)
    send_all(lambda d: d[2] != 0)
    def land(wanted):
        for d, make in everything:
            if wanted(d):
                def arrive(make=make):
                    for c in make():
                        c.wait_recv()
                when(exists(-d[0], -d[1]), arrive)

    first, last = lane8 == 0, lane8 == 127

    def zup(a):
        r = [pltpu.roll(v, 127, 1) for v in a]
        return [jnp.where(last, r[(t + 1) % nt], r[t]) for t in range(nt)]

    def zdown(a):
        r = [pltpu.roll(v, 1, 1) for v in a]
        return [jnp.where(first, r[t - 1], r[t]) for t in range(nt)]

    def zsmooth(a):
        return [(v + v) + (w + q) for v, w, q in zip(a, zup(a), zdown(a))]

    def field_plane(x, _):
        for r in starts:
            here = slice(r, r + 8)
            m = [[V[3 + c, t, x, here, :] for c in range(3)] for t in range(nt)]
            u, d = [], [[[None] * 3 for _ in range(3)] for _ in range(nt)]
            for i in range(3):
                mid = [V[i, t, x, here, :] for t in range(nt)]
                u.append(mid)
                hi, lo = zup(mid), zdown(mid)
                for t in range(nt):
                    above, below = V[i, t, x, r + 1 : r + 9, :], V[i, t, x, r - 1 : r + 7, :]
                    Gv[i, t, x, here, :] = (mid[t] + mid[t]) + (above + below)
                    d[t][i][0] = m[t][0] * (V[i, t, x + 1, here, :] - V[i, t, x - 1, here, :])
                    d[t][i][1] = m[t][1] * (above - below)
                    d[t][i][2] = m[t][2] * (hi[t] - lo[t])
            for t in range(nt):
                f, square = tensor(d[t])
                mag = root(0.5 * square)
                dq = jnp.exp2((-2.0 / 3.0) * jnp.log2(m[t][0] * m[t][1] * m[t][2]))
                Q[t, x, here, :] = dq
                M[t, x, here, :] = dq * mag
                for k, (a, b) in enumerate(pairs):
                    F[k, t, x, here, :] = u[a][t] * u[b][t]
                    F[6 + k, t, x, here, :] = mag * f[k]
        return 0

    def velocity_plane(x, _):
        for c in range(3):
            for t in range(nt):
                for r in starts:
                    mid = V[c, t, x, r : r + 8, :]
                    Gv[c, t, x, r : r + 8, :] = (mid + mid) + (V[c, t, x, r - 1 : r + 7, :] + V[c, t, x, r + 1 : r + 9, :])
        return 0

    zi = lax.broadcasted_iota(jnp.int32, (nz, nz), 0)
    zj = lax.broadcasted_iota(jnp.int32, (nz, nz), 1)
    gap = jnp.abs(zi - zj)
    W[...] = jnp.where(gap == 0, 2.0, jnp.where((gap == 1) | (gap == nz - 1), 1.0, 0.0)).astype(jnp.bfloat16)

    def banded(a):
        w = W[...]
        hi = a.astype(jnp.bfloat16)
        rest = a - hi.astype(jnp.float32)
        mid = rest.astype(jnp.bfloat16)
        low = (rest - mid.astype(jnp.float32)).astype(jnp.bfloat16)
        n = a.shape[0]
        out = jnp.dot(jnp.concatenate([hi, mid, low], axis=0), w, preferred_element_type=jnp.float32)
        return out[0:n] + (out[n : 2 * n] + out[2 * n :])

    def smooth_plane(x, _):
        for k0 in (0,):
            s = []
            for k in range(12):
                row = []
                for t in range(nt):
                    mid = F[k, t, x, 2 : 2 + ny, :]
                    row.append((mid + mid) + (F[k, t, x, 1 : 1 + ny, :] + F[k, t, x, 3 : 3 + ny, :]))
                s.append(jnp.concatenate(row, axis=1))
            s = banded(jnp.concatenate(s, axis=0))
            for k in range(12):
                for t in range(nt):
                    G[k, t, x, 0:ny, :] = s[(k - k0) * ny : (k - k0 + 1) * ny, 128 * t : 128 * t + 128]
        return 0

    has_lo = jnp.where(iy > 0, 0.125, 0.0)
    has_hi = jnp.where(iy < NY - 1, 0.125, 0.0)
    rows8 = lax.broadcasted_iota(jnp.int32, (8, 128), 0)

    def row_scale(r):
        idx = rows8 + r
        return jnp.where(idx < 2, has_lo, jnp.where(idx < ny + 2, 0.125, has_hi))

    def hat_plane(x, _):
        inside = jnp.where((x == 1) & (ix == 0), 0.0, jnp.where((x == nx + 2) & (ix == NX - 1), 0.0, 1.0))
        for r in starts:
            scale = row_scale(r) * inside
            for c in range(3):
                s = []
                for t in range(nt):
                    mid = Gv[c, t, x, r : r + 8, :]
                    s.append((mid + mid) + (Gv[c, t, x - 1, r : r + 8, :] + Gv[c, t, x + 1, r : r + 8, :]))
                s = zsmooth(s)
                for t in range(nt):
                    H[c, t, x, r : r + 8, :] = s[t] * scale
        return 0

    keep = [None] * nt
    keep[0] = lane8 >= 2
    keep[nt - 1] = (lane8 < 126) if nt > 1 else (lane8 >= 2) & (lane8 < 126)

    def line_plane(x, sums):
        out = []
        for b, r in enumerate(range(0, ny, 8)):
            here = slice(r + 2, r + 10)
            filtered = []
            for k in range(12):
                s = []
                for t in range(nt):
                    mid = G[k, t, x, r : r + 8, :]
                    s.append((mid + mid) + (G[k, t, x - 1, r : r + 8, :] + G[k, t, x + 1, r : r + 8, :]))
                filtered.append(s)
            hat, d = [], [[[None] * 3 for _ in range(3)] for _ in range(nt)]
            m = [[V[3 + c, t, x, here, :] for c in range(3)] for t in range(nt)]
            for i in range(3):
                mid = [H[i, t, x, here, :] for t in range(nt)]
                hat.append(mid)
                hi, lo = zup(mid), zdown(mid)
                for t in range(nt):
                    d[t][i][0] = m[t][0] * (H[i, t, x + 1, here, :] - H[i, t, x - 1, here, :])
                    d[t][i][1] = m[t][1] * (H[i, t, x, r + 3 : r + 11, :] - H[i, t, x, r + 1 : r + 9, :])
                    d[t][i][2] = m[t][2] * (hi[t] - lo[t])
            num = den = 0.0
            for t in range(nt):
                n, e = model_sums([filtered[k][t] for k in range(6)], [filtered[6 + k][t] for k in range(6)], [h[t] for h in hat], d[t], Q[t, x, here, :])
                if keep[t] is not None:
                    n, e = jnp.where(keep[t], n, 0.0), jnp.where(keep[t], e, 0.0)
                num, den = num + n, den + e
            num = jnp.sum(num, axis=1, keepdims=True)
            den = jnp.sum(den, axis=1, keepdims=True)
            acc = jnp.where(lane8 == G6 * x + 2, num, sums[b])
            out.append(jnp.where(lane8 == G6 * x + 4, den, acc))
        return tuple(out)

    def land_chunk(c):
        for n, (dx, dy) in enumerate(plane_offsets):
            if dx == 0:
                def arrive(n=n):
                    for cp in plane_copies(n, c):
                        cp.wait_recv()
                when(exists(0, -dy), arrive)

    def land_x():
        land(lambda d: d[0] != 0 and d[2] == 0)

    def order(i):
        return jnp.where(i < nx, i + 3, nx + 2 - i)

    def line_order(i):
        return jnp.where(i < nx - 2, i + 4, nx + 1 - i)

    def step(i, sums):
        for at, wait in waits:
            pl.when(i == at)(wait)
        sums = line_plane(line_order(i - 5), sums)
        hat_plane(order(i - 2), 0)
        smooth_plane(order(i - 1), 0)
        field_plane(order(i), 0)
        return sums

    def far_velocity():
        lax.fori_loop(0, 2, lambda i, c: velocity_plane(i * (nx + 3), c), 0)

    def land_far():
        land_x()
        far_velocity()

    need = [0] + [chunk * c - 2 for c in range(1, chunks)]
    waits = [(at, functools.partial(land_chunk, c)) for c, at in enumerate(need) if at >= 5] + [(nx - 2, land_far)]
    sums = tuple(jnp.zeros((8, 128), jnp.float32) for _ in range(0, ny, 8))
    land_chunk(0)
    velocity_plane(2, 0)
    def early(i, c):
        for q, at in enumerate(need):
            if 0 < at < 5:
                pl.when(i == at)(functools.partial(land_chunk, q))
        return field_plane(order(i), c)
    lax.fori_loop(0, 5, early, 0)
    lax.fori_loop(0, 4, lambda i, c: smooth_plane(order(i), c), 0)
    lax.fori_loop(0, 3, lambda i, c: hat_plane(order(i), c), 0)
    sums = lax.fori_loop(5, nx + 2, step, sums)
    smooth_plane(order(nx + 1), 0)
    lax.fori_loop(nx, nx + 2, lambda i, c: hat_plane(order(i), c), 0)
    sums = lax.fori_loop(nx - 3, nx, lambda i, c: line_plane(line_order(i), c), sums)
    land(lambda d: d[2] != 0)
    for n, (dx, dy) in enumerate(plane_offsets):
        if dx == 0:
            when(exists(dx, -dy), lambda n=n: edge_rows(n).wait_recv())

    yr = ny + 8
    lane_r = lax.broadcasted_iota(jnp.int32, (yr, 128), 1)
    group_r = (lane_r * 43) >> 8
    inner_r = lane_r - G6 * group_r
    rows_r = lax.broadcasted_iota(jnp.int32, (yr, 128), 0)
    outside = ((group_r == 1) & (ix == 0)) | ((group_r == nx + 2) & (ix == NX - 1))
    outside = outside | ((rows_r < 2) & (iy == 0)) | ((rows_r >= ny + 2) & (iy == NY - 1))
    scale_r = jnp.where(outside, 0.0, 0.125)
    enum, eden = 0.0, 0.0
    fixes = []
    for s in range(2):
        mixed = []
        for k in range(2):
            far = jnp.where(lane_r < 2 * G6, lroll(R[1 - s, 0, k], -G6 * nx), R[1 - s, 1, k])
            mixed.append(jnp.where(lane_r >= G6 * (nx + 2), lroll(R[1 - s, 2, k], G6 * nx), far))
        fields = []
        for f in range(6):
            own = TE[s, f]
            for p in (0, 1, nx + 2, nx + 3):
                if f >= 3 and p in (0, nx + 3):
                    continue
                tile = V[f, 0 if s == 0 else nt - 1, p]
                own = jnp.where(group_r == p, lroll(tile, G6 * p - (0 if s == 0 else 122)), own)
            c = f % 3
            if s == 0:
                fields.append(jnp.where(inner_r < 2, lroll(mixed[f // 3], -2 * c), lroll(own, 2)))
            else:
                fields.append(jnp.where(inner_r >= 4, lroll(mixed[f // 3], 4 - 2 * c), lroll(own, -2)))
        u, m = fields[0:3], fields[3:6]
        for f in range(6):
            E[s, f] = fields[f]
        def shift(a, n):
            return lroll(a, -n)
        d = [[None] * 3 for _ in range(3)]
        for i in range(3):
            d[i][0] = m[0] * (shift(u[i], G6) - shift(u[i], -G6))
            d[i][1] = m[1] * (pltpu.roll(u[i], yr - 1, 0) - pltpu.roll(u[i], 1, 0))
            d[i][2] = m[2] * (shift(u[i], 1) - shift(u[i], -1))
        f, square = tensor(d)
        mag = root(0.5 * square)
        dq = jnp.exp2((-2.0 / 3.0) * jnp.log2(m[0] * m[1] * m[2]))
        EF[s, 15] = dq
        EF[s, 16] = dq * mag
        for c in range(3):
            EF[s, 12 + c] = u[c]
        for k, (a, b) in enumerate(pairs):
            EF[s, k] = u[a] * u[b]
            EF[s, 6 + k] = mag * f[k]
        def lanes_smooth(a):
            b = (a + a) + (shift(a, G6) + shift(a, -G6))
            return (b + b) + (shift(b, 1) + shift(b, -1))
        for c in range(3):
            y = (u[c] + u[c]) + (pltpu.roll(u[c], yr - 1, 0) + pltpu.roll(u[c], 1, 0))
            EG[s, c] = lanes_smooth(y) * scale_r
        own = slice(2, 2 + ny)
        filtered = []
        for k in range(12):
            mid = EF[s, k, own, :]
            filtered.append(lanes_smooth((mid + mid) + (EF[s, k, 1 : 1 + ny, :] + EF[s, k, 3 : 3 + ny, :])))
        hat, dh = [], [[None] * 3 for _ in range(3)]
        me = [E[s, 3 + c, own, :] for c in range(3)]
        for i in range(3):
            mid = EG[s, i, own, :]
            hat.append(mid)
            dh[i][0] = me[0] * (shift(mid, G6) - shift(mid, -G6))
            dh[i][1] = me[1] * (EG[s, i, 3 : 3 + ny, :] - EG[s, i, 1 : 1 + ny, :])
            dh[i][2] = me[2] * (shift(mid, 1) - shift(mid, -1))
        n, e = model_sums(filtered[0:6], filtered[6:12], hat, dh, EF[s, 15, own, :])
        enum, eden = enum + n, eden + e
    enum = enum + lroll(enum, -1)
    eden = lroll(eden + lroll(eden, -1), 2)
    used = (group >= 2) & (group < nx + 2)
    extra = jnp.where(used & (inner == 2), enum, jnp.where(used & (inner == 4), eden, 0.0))
    LS[iz] = jnp.concatenate(sums, axis=0) + extra

    def line_copy(o):
        return pltpu.make_async_remote_copy(
            src_ref=LS.at[iz], dst_ref=LS.at[iz], send_sem=lsend.at[o - 1], recv_sem=lrecv.at[o - 1],
            device_id=(ix, iy, lax.rem(iz + o, NZ)), device_id_type=MESH)
    def line_landing(o):
        src = lax.rem(iz - o + NZ, NZ)
        return pltpu.make_async_remote_copy(
            src_ref=LS.at[src], dst_ref=LS.at[src], send_sem=lsend.at[o - 1], recv_sem=lrecv.at[o - 1],
            device_id=(ix, iy, lax.rem(iz + o, NZ)), device_id_type=MESH)
    for o in range(1, NZ):
        line_copy(o).start()

    lo_fix, hi_fix = EF[0, 16, 2 : 2 + ny, :], EF[1, 16, 2 : 2 + ny, :]
    def weight_plane(x, _):
        p = x + 2
        for t in range(nt):
            tile = M[t, p, 2 : 2 + ny, :]
            if t == 0:
                tile = jnp.where(lane == 0, pltpu.roll(lo_fix, 126 - G6 * p, 1), tile)
            if t == nt - 1:
                tile = jnp.where(lane == 127, pltpu.roll(hi_fix, 124 - G6 * p, 1), tile)
            D[x, :, 128 * t : 128 * t + 128] = tile
        return 0
    lax.fori_loop(0, nx, weight_plane, 0, unroll=4)
    for o in range(1, NZ):
        line_landing(o).wait_recv()
    total = LS[0]
    for o in range(1, NZ):
        total = total + LS[o]
    unit = 4096.0 * nz * NZ
    coef = (total / unit) / (lroll(total, -2) / unit + eps_line)
    masked = jnp.where(used & (inner == 2), coef, -jnp.inf)
    here_max = masked[0:8]
    for r in range(8, ny, 8):
        here_max = jnp.maximum(here_max, masked[r : r + 8])
    me = ix * NY + iy
    PS[me] = here_max
    def peak_copy(j, a, b, landing):
        tx, ty = lax.rem(ix + a, NX), lax.rem(iy + b, NY)
        slot = me
        if landing:
            slot = lax.rem(ix - a + NX, NX) * NY + lax.rem(iy - b + NY, NY)
        return pltpu.make_async_remote_copy(
            src_ref=PS.at[slot], dst_ref=PS.at[slot], send_sem=psend.at[j], recv_sem=precv.at[j],
            device_id=(tx, ty, iz), device_id_type=MESH)
    for j, (a, b) in enumerate(plane_peers):
        peak_copy(j, a, b, False).start()
    for o in range(1, NZ):
        line_copy(o).wait_send()
    for d, make in everything:
        def left(make=make):
            for c in make():
                c.wait_send()
        when(exists(d[0], d[1]), left)
    for n, (dx, dy) in enumerate(plane_offsets):
        if dx == 0:
            when(exists(dx, dy), lambda n=n: edge_rows(n).wait_send())
    for j, (a, b) in enumerate(plane_peers):
        peak_copy(j, a, b, True).wait_recv()
    peak = PS[0]
    for j in range(1, NX * NY):
        peak = jnp.maximum(peak, PS[j])
    coef_out[...] = jnp.minimum(coef, 0.5 * jnp.max(peak, axis=(0, 1), keepdims=True))
    for j, (a, b) in enumerate(plane_peers):
        peak_copy(j, a, b, False).wait_send()


def scale_kernel(D, coef, visc, coef_out):
    nx, ny = visc.shape[:2]
    lane = lax.broadcasted_iota(jnp.int32, (ny, 128), 1)
    table = coef[...]
    turned = table.T
    for x in range(nx):
        at = G6 * (x + 2) + 2
        column = jnp.sum(jnp.where(lane == at, table, 0.0), axis=1, keepdims=True)
        visc[x] = D[x] * column
        coef_out[x : x + 1, :] = turned[at : at + 1, :]


def per_device(sizes, velocity, metric):
    nx, ny, nz = velocity.shape[1:]
    NX, NY, NZ = sizes
    assert nz % 128 == 0 and ny % 8 == 0 and G6 * (nx + 4) <= 128 and nx >= 6
    nt, pa, yr = nz // 128, nx + 4 + (nx + 1) % 2, ny + 8
    f32 = jnp.float32
    copies = len(span_offsets) + (2 * chunks + 1) * len(plane_offsets)
    dmag, coef = pl.pallas_call(
        functools.partial(kernel, sizes),
        out_shape=(pltpu.VMEM((nx, ny, nz), f32), pltpu.VMEM((ny, 128), f32)),
        in_specs=[pl.BlockSpec(memory_space=pltpu.HBM)] * 2,
        out_specs=(pl.BlockSpec(memory_space=pltpu.VMEM), pl.BlockSpec(memory_space=pltpu.VMEM)),
        scratch_shapes=[
            pltpu.VMEM((6, nt, pa, yr, 128), f32),
            pltpu.VMEM((3, nt, pa, yr, 128), f32),
            pltpu.VMEM((12, nt, pa, yr, 128), f32),
            pltpu.VMEM((3, nt, pa, yr, 128), f32),
            pltpu.VMEM((nt, pa, yr, 128), f32),
            pltpu.VMEM((nt, pa, yr, 128), f32),
            pltpu.VMEM((12, nt, pa, yr, 128), f32),
            pltpu.VMEM((2, 6, yr, 128), f32),
            pltpu.VMEM((2, 6, yr, 128), f32),
            pltpu.VMEM((2, 17, yr, 128), f32),
            pltpu.VMEM((2, 3, yr, 128), f32),
            pltpu.VMEM((2, 2, ny, 128), f32),
            pltpu.VMEM((2, 3, 2, yr, 128), f32),
            pltpu.VMEM((NZ, ny, 128), f32),
            pltpu.VMEM((NX * NY, 8, 128), f32),
            pltpu.VMEM((nz, nz), jnp.bfloat16),
            pltpu.SemaphoreType.REGULAR((2,)),
            pltpu.SemaphoreType.DMA((2 * nt + 1,)),
            pltpu.SemaphoreType.DMA((copies,)),
            pltpu.SemaphoreType.DMA((copies,)),
            pltpu.SemaphoreType.DMA((NZ,)),
            pltpu.SemaphoreType.DMA((NZ,)),
            pltpu.SemaphoreType.DMA((NX * NY,)),
            pltpu.SemaphoreType.DMA((NX * NY,)),
        ],
        compiler_params=pltpu.CompilerParams(collective_id=0, has_side_effects=True, vmem_limit_bytes=67043328 - 600 * 1024),
    )(velocity, metric)
    return pl.pallas_call(
        scale_kernel,
        out_shape=(jax.ShapeDtypeStruct((nx, ny, nz), f32), jax.ShapeDtypeStruct((nx, ny), f32)),
        in_specs=[pl.BlockSpec(memory_space=pltpu.VMEM)] * 2,
        out_specs=(pl.BlockSpec(memory_space=pltpu.VMEM),) * 2,
        compiler_params=pltpu.CompilerParams(vmem_limit_bytes=4 * 1024 * 1024),
    )(dmag, coef)


def solution(mesh):
    sizes = (mesh.shape["gx"], mesh.shape["gy"], mesh.shape["gz"])
    return jax.shard_map(
        functools.partial(per_device, sizes),
        mesh=mesh,
        in_specs=(P(None, "gx", "gy", "gz"), P(None, "gx", "gy", "gz")),
        out_specs=(P("gx", "gy", "gz"), P("gx", "gy")),
        check_vma=False,
    )
```

```python
import functools

import jax
import jax.numpy as jnp
from jax import lax
from jax.experimental import pallas as pl
from jax.experimental.pallas import tpu as pltpu
from jax.sharding import PartitionSpec as P

MESH = pl.DeviceIdType.MESH
pairs = ((0, 0), (1, 1), (2, 2), (0, 1), (0, 2), (1, 2))
eps_line = 1e-06
smallest = 1.1754944e-38
plane_offsets = [(dx, dy) for dx in (0, 1, -1) for dy in (0, 1, -1) if (dx, dy) != (0, 0)]
span_offsets = [(dx, dy, dz) for dz in (1, -1) for dx in (0, 1, -1) for dy in (0, 1, -1)]
chunks = 4
G6 = 6


def root(s):
    return s * lax.rsqrt(jnp.maximum(s, smallest))


def tensor(d):
    f = [d[a][b] if a == b else d[a][b] + d[b][a] for a, b in pairs]
    square = (f[0] * f[0] + f[1] * f[1] + f[2] * f[2]) + 0.5 * (f[3] * f[3] + f[4] * f[4] + f[5] * f[5])
    return f, square


def model_sums(vv, ms, hat, dh, dq):
    f, square = tensor(dh)
    mh = root(8.0 * square)
    num = den = off = None
    for k, (a, b) in enumerate(pairs):
        leonard = vv[k] - hat[a] * hat[b]
        model = ms[k] - mh * f[k]
        n, m2 = leonard * model, model * model
        num = n if num is None else num + n
        if a == b:
            den = m2 if den is None else den + m2
        else:
            off = m2 if off is None else off + m2
    return num * dq, (den + 0.5 * off) * (dq * dq)


def kernel(sizes, vel, met, D, coef_out, V, Gv, G, H, Q, M, F, TE, E, EF, EG, PK, R, LS, PS, W, W2, token, sem_in, send, recv, lsend, lrecv, psend, precv):
    NX, NY, NZ = sizes
    nx, ny, nz = vel.shape[1:]
    nt = nz // 128
    px = nx + 4
    starts = list(range(1, ny - 6, 8)) + [ny - 5]
    ix, iy, iz = lax.axis_index("gx"), lax.axis_index("gy"), lax.axis_index("gz")

    loads = []
    for k, src in enumerate((vel, met)):
        for t in range(nt):
            loads.append(pltpu.make_async_copy(
                src.at[:, :, :, 128 * t : 128 * t + 128],
                V.at[3 * k : 3 * k + 3, t, 2 : 2 + nx, 2 : 2 + ny, :],
                sem_in.at[k * nt + t]))
    for c in loads:
        c.start()

    def there(delta, i, n):
        return None if delta == 0 else (i + delta >= 0) & (i + delta < n)

    def exists(dx, dy):
        a, b = there(dx, ix, NX), there(dy, iy, NY)
        if a is None:
            return b
        return a if b is None else a & b

    def when(cond, fn):
        if cond is None:
            fn()
        else:
            pl.when(cond)(fn)

    def dev(d):
        return (ix + d[0], iy + d[1], lax.rem(iz + d[2] + NZ, NZ))

    barrier = pltpu.get_barrier_semaphore()
    expected = jnp.int32(0)
    plane_peers = [(a, b) for a in range(NX) for b in range(NY) if (a, b) != (0, 0)]
    for a, b in plane_peers:
        pl.semaphore_signal(barrier, inc=1, device_id=(lax.rem(ix + a, NX), lax.rem(iy + b, NY), iz), device_id_type=MESH)
    expected = expected + len(plane_peers)
    for dz in (1, -1):
        ok = there(dz, iz, NZ)
        pl.when(ok)(lambda dz=dz: pl.semaphore_signal(barrier, inc=1, device_id=(ix, iy, iz + dz), device_id_type=MESH))
        expected = expected + ok.astype(jnp.int32)

    def tell(dz):
        pl.when(there(dz, iz, NZ))(lambda: pl.semaphore_signal(token.at[(dz + 1) // 2], inc=1, device_id=(ix, iy, iz + dz), device_id_type=MESH))

    def relay(dz):
        def hear():
            pl.semaphore_wait(token.at[(dz + 1) // 2], 1)
            tell(dz)
        pl.when(there(-dz, iz, NZ))(hear)

    z2 = jnp.zeros((2, 128), jnp.float32)
    for dx, p0 in ((-1, 0), (1, nx + 2)):
        def clear_planes(dx=dx, p0=p0):
            for f in range(6):
                for t in range(nt):
                    for p in (p0, p0 + 1):
                        V[f, t, p] = jnp.zeros((ny + 8, 128), jnp.float32)
            for s in range(2):
                for k in range(2):
                    R[s, dx + 1, k] = jnp.zeros((ny + 8, 128), jnp.float32)
        pl.when(jnp.logical_not(there(dx, ix, NX)))(clear_planes)
    for dy, r0 in ((-1, 0), (1, ny + 2)):
        def clear_rows(r0=r0):
            def body(p, _):
                for f in range(6):
                    for t in range(nt):
                        V[f, t, p, r0 : r0 + 2, :] = z2
                return 0
            lax.fori_loop(0, px, body, 0)
            for s in range(2):
                for f in range(6):
                    TE[s, f, r0 : r0 + 2, :] = z2
                for dxi in range(3):
                    for k in range(2):
                        R[s, dxi, k, r0 : r0 + 2, :] = z2
        pl.when(jnp.logical_not(there(dy, iy, NY)))(clear_rows)

    pl.semaphore_wait(barrier, expected)
    for dz in (1, -1):
        pl.when(jnp.logical_not(there(-dz, iz, NZ)))(functools.partial(tell, dz))
    for c in loads:
        c.wait()

    lane = lax.broadcasted_iota(jnp.int32, (ny, 128), 1)
    group = (lane * 43) >> 8
    inner = lane - G6 * group
    lane8, group8, inner8 = lane[0:8], group[0:8], inner[0:8]

    def lroll(a, s):
        s = s % 128
        return pltpu.roll(a, s, 1) if s else a


    def span_x(dx, deep):
        if dx == 0:
            return (2, 2, nx)
        if dx == 1:
            return (nx, 0, 2) if deep else (nx + 1, 1, 1)
        return (2, nx + 2, 2) if deep else (2, nx + 2, 1)

    def span_y(dy, deep):
        if dy == 0:
            return (2, 2, ny)
        if dy == 1:
            return (ny, 0, 2) if deep else (ny + 1, 1, 1)
        return (2, ny + 2, 2) if deep else (2, ny + 2, 1)

    def remote(src, dst, j, d):
        return pltpu.make_async_remote_copy(src_ref=src, dst_ref=dst, send_sem=send.at[j], recv_sem=recv.at[j], device_id=dev(d), device_id_type=MESH)

    def span_copy(n):
        dx, dy, dz = d = span_offsets[n]
        s = 1 if dz == 1 else 0
        ys, yd, yn = span_y(dy, True)
        return remote(PK.at[s, :, ys - 2 : ys - 2 + yn, :], R.at[s, 1 - dx, :, yd : yd + yn, :], n, d)

    chunk = nx // chunks

    def plane_copies(n, part=None):
        dx, dy = plane_offsets[n]
        d = (dx, dy, 0)
        base = len(span_offsets) + (2 * chunks + 1) * n
        out = []
        for c in range(chunks if dx == 0 else 1):
            if part is not None and c != part:
                continue
            for k in range(2):
                xs, xd, xn = span_x(dx, k == 0)
                if dx == 0:
                    xs, xd, xn = 2 + c * chunk, 2 + c * chunk, chunk
                ys, yd, yn = span_y(dy, k == 0)
                f0 = 3 * k
                out.append(remote(V.at[f0 : f0 + 3, :, xs : xs + xn, ys : ys + yn, :], V.at[f0 : f0 + 3, :, xd : xd + xn, yd : yd + yn, :], base + 2 * c + k, d))
        return out

    def edge_rows(n):
        dx, dy = plane_offsets[n]
        ys, yd, yn = span_y(dy, True)
        return remote(TE.at[:, :, ys : ys + yn, :], TE.at[:, :, yd : yd + yn, :], len(span_offsets) + (2 * chunks + 1) * n + 2 * chunks, (dx, dy, 0))

    everything = [(d, (lambda n=n: [span_copy(n)])) for n, d in enumerate(span_offsets)]
    everything += [((dx, dy, 0), (lambda n=n: plane_copies(n))) for n, (dx, dy) in enumerate(plane_offsets)]
    def send_all(wanted):
        for d, make in everything:
            if wanted(d):
                def go(make=make):
                    for c in make():
                        c.start()
                when(exists(d[0], d[1]), go)

    def send_chunk(c):
        for n, (dx, dy) in enumerate(plane_offsets):
            if dx == 0:
                def go(n=n):
                    for cp in plane_copies(n, c):
                        cp.start()
                when(exists(0, dy), go)

    send_chunk(0)
    for f in range(6):
        for s in range(2):
            acc = jnp.zeros((ny, 128), jnp.float32)
            for p in range(2, 2 + nx):
                tile = V[f, 0 if s == 0 else nt - 1, p, 2 : 2 + ny, :]
                acc = jnp.where(group == p, lroll(tile, G6 * p - (0 if s == 0 else 122)), acc)
            TE[s, f, 2 : 2 + ny, :] = acc
    for s in range(2):
        for k in range(2):
            parts = [lroll(TE[s, 3 * k + c, 2 : 2 + ny, :], 2 * c - (0 if s == 0 else 4)) for c in range(3)]
            PK[s, k] = jnp.where(inner < 2, parts[0], jnp.where(inner < 4, parts[1], parts[2]))

    for c in range(1, chunks):
        send_chunk(c)
    for n, (dx, dy) in enumerate(plane_offsets):
        if dx == 0:
            when(exists(dx, dy), lambda n=n: edge_rows(n).start())
    send_all(lambda d: d[2] == 0 and d[0] != 0)
    relay(1)
    relay(-1)
    send_all(lambda d: d[2] != 0)
    def land(wanted):
        for d, make in everything:
            if wanted(d):
                def arrive(make=make):
                    for c in make():
                        c.wait_recv()
                when(exists(-d[0], -d[1]), arrive)

    first, last = lane8 == 0, lane8 == 127

    def zup(a):
        r = [pltpu.roll(v, 127, 1) for v in a]
        return [jnp.where(last, r[(t + 1) % nt], r[t]) for t in range(nt)]

    def zdown(a):
        r = [pltpu.roll(v, 1, 1) for v in a]
        return [jnp.where(first, r[t - 1], r[t]) for t in range(nt)]

    def zsmooth(a):
        return [(v + v) + (w + q) for v, w, q in zip(a, zup(a), zdown(a))]

    def field_plane(x, _):
        for r in starts:
            here = slice(r, r + 8)
            m = [[V[3 + c, t, x, here, :] for c in range(3)] for t in range(nt)]
            u, d = [], [[[None] * 3 for _ in range(3)] for _ in range(nt)]
            for i in range(3):
                mid = [V[i, t, x, here, :] for t in range(nt)]
                u.append(mid)
                hi, lo = zup(mid), zdown(mid)
                for t in range(nt):
                    above, below = V[i, t, x, r + 1 : r + 9, :], V[i, t, x, r - 1 : r + 7, :]
                    Gv[i, t, x, here, :] = (mid[t] + mid[t]) + (above + below)
                    d[t][i][0] = m[t][0] * (V[i, t, x + 1, here, :] - V[i, t, x - 1, here, :])
                    d[t][i][1] = m[t][1] * (above - below)
                    d[t][i][2] = m[t][2] * (hi[t] - lo[t])
            for t in range(nt):
                f, square = tensor(d[t])
                mag = root(0.5 * square)
                dq = jnp.exp2((-2.0 / 3.0) * jnp.log2(m[t][0] * m[t][1] * m[t][2]))
                Q[t, x, here, :] = dq
                M[t, x, here, :] = dq * mag
                for k, (a, b) in enumerate(pairs):
                    F[k, t, x, here, :] = u[a][t] * u[b][t]
                    F[6 + k, t, x, here, :] = mag * f[k]
        return 0

    def velocity_plane(x, _):
        for c in range(3):
            for t in range(nt):
                for r in starts:
                    mid = V[c, t, x, r : r + 8, :]
                    Gv[c, t, x, r : r + 8, :] = (mid + mid) + (V[c, t, x, r - 1 : r + 7, :] + V[c, t, x, r + 1 : r + 9, :])
        return 0

    zi = lax.broadcasted_iota(jnp.int32, (nz, nz), 0)
    zj = lax.broadcasted_iota(jnp.int32, (nz, nz), 1)
    gap = jnp.abs(zi - zj)
    W[...] = jnp.where(gap == 0, 2.0, jnp.where((gap == 1) | (gap == nz - 1), 1.0, 0.0)).astype(jnp.bfloat16)

    gap = jnp.abs(zi[0:128, 0:128] - zj[0:128, 0:128])
    W2[...] = jnp.where(gap == 0, 4.0, jnp.where((gap == 1) | (gap == G6), 2.0, jnp.where((gap == G6 - 1) | (gap == G6 + 1), 1.0, 0.0))).astype(jnp.bfloat16)

    def banded(a, w):
        hi = a.astype(jnp.bfloat16)
        rest = a - hi.astype(jnp.float32)
        mid = rest.astype(jnp.bfloat16)
        low = (rest - mid.astype(jnp.float32)).astype(jnp.bfloat16)
        n = a.shape[0]
        out = jnp.dot(jnp.concatenate([hi, mid, low], axis=0), w, preferred_element_type=jnp.float32)
        return out[0:n] + (out[n : 2 * n] + out[2 * n :])

    def smooth_plane(x, _):
        for k0 in (0,):
            s = []
            for k in range(12):
                row = []
                for t in range(nt):
                    mid = F[k, t, x, 2 : 2 + ny, :]
                    row.append((mid + mid) + (F[k, t, x, 1 : 1 + ny, :] + F[k, t, x, 3 : 3 + ny, :]))
                s.append(jnp.concatenate(row, axis=1))
            s = banded(jnp.concatenate(s, axis=0), W[...])
            for k in range(12):
                for t in range(nt):
                    G[k, t, x, 0:ny, :] = s[(k - k0) * ny : (k - k0 + 1) * ny, 128 * t : 128 * t + 128]
        return 0

    has_lo = jnp.where(iy > 0, 0.125, 0.0)
    has_hi = jnp.where(iy < NY - 1, 0.125, 0.0)
    rows8 = lax.broadcasted_iota(jnp.int32, (8, 128), 0)

    def row_scale(r):
        idx = rows8 + r
        return jnp.where(idx < 2, has_lo, jnp.where(idx < ny + 2, 0.125, has_hi))

    def hat_plane(x, _):
        inside = jnp.where((x == 1) & (ix == 0), 0.0, jnp.where((x == nx + 2) & (ix == NX - 1), 0.0, 1.0))
        for r in starts:
            scale = row_scale(r) * inside
            for c in range(3):
                s = []
                for t in range(nt):
                    mid = Gv[c, t, x, r : r + 8, :]
                    s.append((mid + mid) + (Gv[c, t, x - 1, r : r + 8, :] + Gv[c, t, x + 1, r : r + 8, :]))
                s = zsmooth(s)
                for t in range(nt):
                    H[c, t, x, r : r + 8, :] = s[t] * scale
        return 0

    keep = [None] * nt
    keep[0] = lane8 >= 2
    keep[nt - 1] = (lane8 < 126) if nt > 1 else (lane8 >= 2) & (lane8 < 126)

    def line_plane(x, sums):
        out = []
        for b, r in enumerate(range(0, ny, 8)):
            here = slice(r + 2, r + 10)
            filtered = []
            for k in range(12):
                s = []
                for t in range(nt):
                    mid = G[k, t, x, r : r + 8, :]
                    s.append((mid + mid) + (G[k, t, x - 1, r : r + 8, :] + G[k, t, x + 1, r : r + 8, :]))
                filtered.append(s)
            hat, d = [], [[[None] * 3 for _ in range(3)] for _ in range(nt)]
            m = [[V[3 + c, t, x, here, :] for c in range(3)] for t in range(nt)]
            for i in range(3):
                mid = [H[i, t, x, here, :] for t in range(nt)]
                hat.append(mid)
                hi, lo = zup(mid), zdown(mid)
                for t in range(nt):
                    d[t][i][0] = m[t][0] * (H[i, t, x + 1, here, :] - H[i, t, x - 1, here, :])
                    d[t][i][1] = m[t][1] * (H[i, t, x, r + 3 : r + 11, :] - H[i, t, x, r + 1 : r + 9, :])
                    d[t][i][2] = m[t][2] * (hi[t] - lo[t])
            num = den = 0.0
            for t in range(nt):
                n, e = model_sums([filtered[k][t] for k in range(6)], [filtered[6 + k][t] for k in range(6)], [h[t] for h in hat], d[t], Q[t, x, here, :])
                if keep[t] is not None:
                    n, e = jnp.where(keep[t], n, 0.0), jnp.where(keep[t], e, 0.0)
                num, den = num + n, den + e
            num = jnp.sum(num, axis=1, keepdims=True)
            den = jnp.sum(den, axis=1, keepdims=True)
            acc = jnp.where(lane8 == G6 * x + 2, num, sums[b])
            out.append(jnp.where(lane8 == G6 * x + 4, den, acc))
        return tuple(out)

    def land_chunk(c):
        for n, (dx, dy) in enumerate(plane_offsets):
            if dx == 0:
                def arrive(n=n):
                    for cp in plane_copies(n, c):
                        cp.wait_recv()
                when(exists(0, -dy), arrive)

    def land_x():
        land(lambda d: d[0] != 0 and d[2] == 0)

    def order(i):
        i = jnp.clip(i, 0, nx + 1)
        return jnp.where(i < nx, i + 3, nx + 2 - i)

    def line_order(i):
        i = jnp.clip(i, 0, nx - 1)
        return jnp.where(i < nx - 2, i + 4, nx + 1 - i)

    def step(i, sums):
        sums = line_plane(line_order(i - 5), sums)
        hat_plane(order(i - 2), 0)
        smooth_plane(order(i - 1), 0)
        field_plane(order(i), 0)
        return sums

    def land_far():
        land_x()
        for p in (0, nx + 3):
            velocity_plane(p, 0)

    waits = [(chunk * c - 2, functools.partial(land_chunk, c)) for c in range(1, chunks)] + [(nx - 2, land_far)]
    sums = tuple(jnp.zeros((8, 128), jnp.float32) for _ in range(0, ny, 8))

    def turn(j, sums):
        def arrivals():
            for at, wait in waits:
                pl.when(j == at)(wait)
        pl.when(lax.rem(j + 2, chunk) == 0)(arrivals)
        return step(j, sums)
    land_chunk(0)
    velocity_plane(2, 0)
    sums = lax.fori_loop(0, nx + 5, turn, sums)
    land(lambda d: d[2] != 0)
    for n, (dx, dy) in enumerate(plane_offsets):
        if dx == 0:
            when(exists(dx, -dy), lambda n=n: edge_rows(n).wait_recv())

    yr = ny + 8
    lane_r = lax.broadcasted_iota(jnp.int32, (yr, 128), 1)
    group_r = (lane_r * 43) >> 8
    inner_r = lane_r - G6 * group_r
    rows_r = lax.broadcasted_iota(jnp.int32, (yr, 128), 0)
    outside = ((group_r == 1) & (ix == 0)) | ((group_r == nx + 2) & (ix == NX - 1))
    outside = outside | ((rows_r < 2) & (iy == 0)) | ((rows_r >= ny + 2) & (iy == NY - 1))
    scale_r = jnp.where(outside, 0.0, 0.125)
    enum, eden = 0.0, 0.0
    fixes = []
    for s in range(2):
        mixed = []
        for k in range(2):
            far = jnp.where(lane_r < 2 * G6, lroll(R[1 - s, 0, k], -G6 * nx), R[1 - s, 1, k])
            mixed.append(jnp.where(lane_r >= G6 * (nx + 2), lroll(R[1 - s, 2, k], G6 * nx), far))
        fields = []
        for f in range(6):
            own = TE[s, f]
            for p in (0, 1, nx + 2, nx + 3):
                if f >= 3 and p in (0, nx + 3):
                    continue
                tile = V[f, 0 if s == 0 else nt - 1, p]
                own = jnp.where(group_r == p, lroll(tile, G6 * p - (0 if s == 0 else 122)), own)
            c = f % 3
            if s == 0:
                fields.append(jnp.where(inner_r < 2, lroll(mixed[f // 3], -2 * c), lroll(own, 2)))
            else:
                fields.append(jnp.where(inner_r >= 4, lroll(mixed[f // 3], 4 - 2 * c), lroll(own, -2)))
        u, m = fields[0:3], fields[3:6]
        for f in range(6):
            E[s, f] = fields[f]
        def shift(a, n):
            return lroll(a, -n)
        d = [[None] * 3 for _ in range(3)]
        for i in range(3):
            d[i][0] = m[0] * (shift(u[i], G6) - shift(u[i], -G6))
            d[i][1] = m[1] * (pltpu.roll(u[i], yr - 1, 0) - pltpu.roll(u[i], 1, 0))
            d[i][2] = m[2] * (shift(u[i], 1) - shift(u[i], -1))
        f, square = tensor(d)
        mag = root(0.5 * square)
        dq = jnp.exp2((-2.0 / 3.0) * jnp.log2(m[0] * m[1] * m[2]))
        EF[s, 15] = dq
        EF[s, 16] = dq * mag
        for c in range(3):
            EF[s, 12 + c] = u[c]
        for k, (a, b) in enumerate(pairs):
            EF[s, k] = u[a] * u[b]
            EF[s, 6 + k] = mag * f[k]
        rows = []
        for c in range(3):
            rows.append((u[c] + u[c]) + (pltpu.roll(u[c], yr - 1, 0) + pltpu.roll(u[c], 1, 0)))
        own = slice(2, 2 + ny)
        for k in range(12):
            mid = EF[s, k, own, :]
            rows.append((mid + mid) + (EF[s, k, 1 : 1 + ny, :] + EF[s, k, 3 : 3 + ny, :]))
        smoothed = banded(jnp.concatenate(rows, axis=0), W2[...])
        for c in range(3):
            EG[s, c] = smoothed[yr * c : yr * (c + 1)] * scale_r
        filtered = [smoothed[3 * yr + ny * k : 3 * yr + ny * (k + 1)] for k in range(12)]
        hat, dh = [], [[None] * 3 for _ in range(3)]
        me = [E[s, 3 + c, own, :] for c in range(3)]
        for i in range(3):
            mid = EG[s, i, own, :]
            hat.append(mid)
            dh[i][0] = me[0] * (shift(mid, G6) - shift(mid, -G6))
            dh[i][1] = me[1] * (EG[s, i, 3 : 3 + ny, :] - EG[s, i, 1 : 1 + ny, :])
            dh[i][2] = me[2] * (shift(mid, 1) - shift(mid, -1))
        n, e = model_sums(filtered[0:6], filtered[6:12], hat, dh, EF[s, 15, own, :])
        enum, eden = enum + n, eden + e
    enum = enum + lroll(enum, -1)
    eden = lroll(eden + lroll(eden, -1), 2)
    used = (group >= 2) & (group < nx + 2)
    extra = jnp.where(used & (inner == 2), enum, jnp.where(used & (inner == 4), eden, 0.0))
    LS[iz] = jnp.concatenate(sums, axis=0) + extra

    def line_copy(o):
        return pltpu.make_async_remote_copy(
            src_ref=LS.at[iz], dst_ref=LS.at[iz], send_sem=lsend.at[o - 1], recv_sem=lrecv.at[o - 1],
            device_id=(ix, iy, lax.rem(iz + o, NZ)), device_id_type=MESH)
    def line_landing(o):
        src = lax.rem(iz - o + NZ, NZ)
        return pltpu.make_async_remote_copy(
            src_ref=LS.at[src], dst_ref=LS.at[src], send_sem=lsend.at[o - 1], recv_sem=lrecv.at[o - 1],
            device_id=(ix, iy, lax.rem(iz + o, NZ)), device_id_type=MESH)
    for o in range(1, NZ):
        line_copy(o).start()

    lo_fix, hi_fix = EF[0, 16, 2 : 2 + ny, :], EF[1, 16, 2 : 2 + ny, :]
    def weight_plane(x, _):
        p = x + 2
        for t in range(nt):
            tile = M[t, p, 2 : 2 + ny, :]
            if t == 0:
                tile = jnp.where(lane == 0, pltpu.roll(lo_fix, 126 - G6 * p, 1), tile)
            if t == nt - 1:
                tile = jnp.where(lane == 127, pltpu.roll(hi_fix, 124 - G6 * p, 1), tile)
            D[x, :, 128 * t : 128 * t + 128] = tile
        return 0
    lax.fori_loop(0, nx, weight_plane, 0, unroll=4)
    for o in range(1, NZ):
        line_landing(o).wait_recv()
    total = LS[0]
    for o in range(1, NZ):
        total = total + LS[o]
    unit = 4096.0 * nz * NZ
    coef = (total / unit) / (lroll(total, -2) / unit + eps_line)
    masked = jnp.where(used & (inner == 2), coef, -jnp.inf)
    here_max = masked[0:8]
    for r in range(8, ny, 8):
        here_max = jnp.maximum(here_max, masked[r : r + 8])
    me = ix * NY + iy
    PS[me] = here_max
    def peak_copy(j, a, b, landing):
        tx, ty = lax.rem(ix + a, NX), lax.rem(iy + b, NY)
        slot = me
        if landing:
            slot = lax.rem(ix - a + NX, NX) * NY + lax.rem(iy - b + NY, NY)
        return pltpu.make_async_remote_copy(
            src_ref=PS.at[slot], dst_ref=PS.at[slot], send_sem=psend.at[j], recv_sem=precv.at[j],
            device_id=(tx, ty, iz), device_id_type=MESH)
    for j, (a, b) in enumerate(plane_peers):
        peak_copy(j, a, b, False).start()
    for o in range(1, NZ):
        line_copy(o).wait_send()
    for d, make in everything:
        def left(make=make):
            for c in make():
                c.wait_send()
        when(exists(d[0], d[1]), left)
    for n, (dx, dy) in enumerate(plane_offsets):
        if dx == 0:
            when(exists(dx, dy), lambda n=n: edge_rows(n).wait_send())
    for j, (a, b) in enumerate(plane_peers):
        peak_copy(j, a, b, True).wait_recv()
    peak = PS[0]
    for j in range(1, NX * NY):
        peak = jnp.maximum(peak, PS[j])
    coef_out[...] = jnp.minimum(coef, 0.5 * jnp.max(peak, axis=(0, 1), keepdims=True))
    for j, (a, b) in enumerate(plane_peers):
        peak_copy(j, a, b, False).wait_send()


def scale_kernel(D, coef, visc, coef_out):
    nx, ny = visc.shape[:2]
    lane = lax.broadcasted_iota(jnp.int32, (ny, 128), 1)
    table = coef[...]
    turned = table.T
    for x in range(nx):
        at = G6 * (x + 2) + 2
        column = jnp.sum(jnp.where(lane == at, table, 0.0), axis=1, keepdims=True)
        visc[x] = D[x] * column
        coef_out[x : x + 1, :] = turned[at : at + 1, :]


def per_device(sizes, velocity, metric):
    nx, ny, nz = velocity.shape[1:]
    NX, NY, NZ = sizes
    assert nz % 128 == 0 and ny % 8 == 0 and G6 * (nx + 4) <= 128 and nx >= 6
    nt, pa, yr = nz // 128, nx + 4 + (nx + 1) % 2, ny + 8
    f32 = jnp.float32
    copies = len(span_offsets) + (2 * chunks + 1) * len(plane_offsets)
    dmag, coef = pl.pallas_call(
        functools.partial(kernel, sizes),
        out_shape=(pltpu.VMEM((nx, ny, nz), f32), pltpu.VMEM((ny, 128), f32)),
        in_specs=[pl.BlockSpec(memory_space=pltpu.HBM)] * 2,
        out_specs=(pl.BlockSpec(memory_space=pltpu.VMEM), pl.BlockSpec(memory_space=pltpu.VMEM)),
        scratch_shapes=[
            pltpu.VMEM((6, nt, pa, yr, 128), f32),
            pltpu.VMEM((3, nt, pa, yr, 128), f32),
            pltpu.VMEM((12, nt, pa, yr, 128), f32),
            pltpu.VMEM((3, nt, pa, yr, 128), f32),
            pltpu.VMEM((nt, pa, yr, 128), f32),
            pltpu.VMEM((nt, pa, yr, 128), f32),
            pltpu.VMEM((12, nt, pa, yr, 128), f32),
            pltpu.VMEM((2, 6, yr, 128), f32),
            pltpu.VMEM((2, 6, yr, 128), f32),
            pltpu.VMEM((2, 17, yr, 128), f32),
            pltpu.VMEM((2, 3, yr, 128), f32),
            pltpu.VMEM((2, 2, ny, 128), f32),
            pltpu.VMEM((2, 3, 2, yr, 128), f32),
            pltpu.VMEM((NZ, ny, 128), f32),
            pltpu.VMEM((NX * NY, 8, 128), f32),
            pltpu.VMEM((nz, nz), jnp.bfloat16),
            pltpu.VMEM((128, 128), jnp.bfloat16),
            pltpu.SemaphoreType.REGULAR((2,)),
            pltpu.SemaphoreType.DMA((2 * nt + 1,)),
            pltpu.SemaphoreType.DMA((copies,)),
            pltpu.SemaphoreType.DMA((copies,)),
            pltpu.SemaphoreType.DMA((NZ,)),
            pltpu.SemaphoreType.DMA((NZ,)),
            pltpu.SemaphoreType.DMA((NX * NY,)),
            pltpu.SemaphoreType.DMA((NX * NY,)),
        ],
        compiler_params=pltpu.CompilerParams(collective_id=0, has_side_effects=True, vmem_limit_bytes=67043328 - 600 * 1024),
    )(velocity, metric)
    return pl.pallas_call(
        scale_kernel,
        out_shape=(jax.ShapeDtypeStruct((nx, ny, nz), f32), jax.ShapeDtypeStruct((nx, ny), f32)),
        in_specs=[pl.BlockSpec(memory_space=pltpu.VMEM)] * 2,
        out_specs=(pl.BlockSpec(memory_space=pltpu.VMEM),) * 2,
        compiler_params=pltpu.CompilerParams(vmem_limit_bytes=4 * 1024 * 1024),
    )(dmag, coef)


def solution(mesh):
    sizes = (mesh.shape["gx"], mesh.shape["gy"], mesh.shape["gz"])
    return jax.shard_map(
        functools.partial(per_device, sizes),
        mesh=mesh,
        in_specs=(P(None, "gx", "gy", "gz"), P(None, "gx", "gy", "gz")),
        out_specs=(P("gx", "gy", "gz"), P("gx", "gy")),
        check_vma=False,
    )
```

```python
import functools

import jax
import jax.numpy as jnp
from jax import lax
from jax.experimental import pallas as pl
from jax.experimental.pallas import tpu as pltpu
from jax.sharding import PartitionSpec as P

MESH = pl.DeviceIdType.MESH
pairs = ((0, 0), (1, 1), (2, 2), (0, 1), (0, 2), (1, 2))
eps_line = 1e-06
smallest = 1.1754944e-38
plane_offsets = [(dx, dy) for dx in (0, 1, -1) for dy in (0, 1, -1) if (dx, dy) != (0, 0)]
span_offsets = [(dx, dy, dz) for dz in (1, -1) for dx in (0, 1, -1) for dy in (0, 1, -1)]
chunks = 4
G6 = 6


def root(s):
    return s * lax.rsqrt(jnp.maximum(s, smallest))


def tensor(d):
    f = [d[a][b] if a == b else d[a][b] + d[b][a] for a, b in pairs]
    square = (f[0] * f[0] + f[1] * f[1] + f[2] * f[2]) + 0.5 * (f[3] * f[3] + f[4] * f[4] + f[5] * f[5])
    return f, square


def model_sums(vv, ms, hat, dh, dq):
    f, square = tensor(dh)
    mh = root(8.0 * square)
    num = den = off = None
    for k, (a, b) in enumerate(pairs):
        leonard = vv[k] - hat[a] * hat[b]
        model = ms[k] - mh * f[k]
        n, m2 = leonard * model, model * model
        num = n if num is None else num + n
        if a == b:
            den = m2 if den is None else den + m2
        else:
            off = m2 if off is None else off + m2
    return num * dq, (den + 0.5 * off) * (dq * dq)


def kernel(sizes, vel, met, D, cols, turned, half, V, Gv, G, H, Q, M, F, TE, E, EF, EG, PK, R, LS, PS, W, W2, token, sem_in, send, recv, lsend, lrecv, psend, precv):
    NX, NY, NZ = sizes
    nx, ny, nz = vel.shape[1:]
    nt = nz // 128
    px = nx + 4
    starts = list(range(1, ny - 6, 8)) + [ny - 5]
    ix, iy, iz = lax.axis_index("gx"), lax.axis_index("gy"), lax.axis_index("gz")

    chunk = nx // chunks
    loads = []
    for x0, x1 in ((0, chunk), (chunk, nx)):
        part = []
        for k, src in enumerate((vel, met)):
            for t in range(nt):
                part.append(pltpu.make_async_copy(
                    src.at[:, x0:x1, :, 128 * t : 128 * t + 128],
                    V.at[3 * k : 3 * k + 3, t, 2 + x0 : 2 + x1, 2 : 2 + ny, :],
                    sem_in.at[len(loads) * 2 * nt + len(part)]))
        loads.append(part)
    for c in loads[0] + loads[1]:
        c.start()

    def there(delta, i, n):
        return None if delta == 0 else (i + delta >= 0) & (i + delta < n)

    def exists(dx, dy):
        a, b = there(dx, ix, NX), there(dy, iy, NY)
        if a is None:
            return b
        return a if b is None else a & b

    def when(cond, fn):
        if cond is None:
            fn()
        else:
            pl.when(cond)(fn)

    def dev(d):
        return (ix + d[0], iy + d[1], lax.rem(iz + d[2] + NZ, NZ))

    barrier = pltpu.get_barrier_semaphore()
    expected = jnp.int32(0)
    plane_peers = [(a, b) for a in range(NX) for b in range(NY) if (a, b) != (0, 0)]
    for a, b in plane_peers:
        pl.semaphore_signal(barrier, inc=1, device_id=(lax.rem(ix + a, NX), lax.rem(iy + b, NY), iz), device_id_type=MESH)
    expected = expected + len(plane_peers)
    for dz in (1, -1):
        ok = there(dz, iz, NZ)
        pl.when(ok)(lambda dz=dz: pl.semaphore_signal(barrier, inc=1, device_id=(ix, iy, iz + dz), device_id_type=MESH))
        expected = expected + ok.astype(jnp.int32)

    def tell(dz):
        pl.when(there(dz, iz, NZ))(lambda: pl.semaphore_signal(token.at[(dz + 1) // 2], inc=1, device_id=(ix, iy, iz + dz), device_id_type=MESH))

    def relay(dz):
        def hear():
            pl.semaphore_wait(token.at[(dz + 1) // 2], 1)
            tell(dz)
        pl.when(there(-dz, iz, NZ))(hear)

    z2 = jnp.zeros((2, 128), jnp.float32)
    for dx, p0 in ((-1, 0), (1, nx + 2)):
        def clear_planes(dx=dx, p0=p0):
            for f in range(6):
                for t in range(nt):
                    for p in (p0, p0 + 1):
                        V[f, t, p] = jnp.zeros((ny + 8, 128), jnp.float32)
            for s in range(2):
                for k in range(2):
                    R[s, dx + 1, k] = jnp.zeros((ny + 8, 128), jnp.float32)
        pl.when(jnp.logical_not(there(dx, ix, NX)))(clear_planes)
    for dy, r0 in ((-1, 0), (1, ny + 2)):
        def clear_rows(r0=r0):
            def body(p, _):
                for f in range(6):
                    for t in range(nt):
                        V[f, t, p, r0 : r0 + 2, :] = z2
                return 0
            lax.fori_loop(0, px, body, 0)
            for s in range(2):
                for f in range(6):
                    TE[s, f, r0 : r0 + 2, :] = z2
                for dxi in range(3):
                    for k in range(2):
                        R[s, dxi, k, r0 : r0 + 2, :] = z2
        pl.when(jnp.logical_not(there(dy, iy, NY)))(clear_rows)

    pl.semaphore_wait(barrier, expected)
    for dz in (1, -1):
        pl.when(jnp.logical_not(there(-dz, iz, NZ)))(functools.partial(tell, dz))
    for c in loads[0]:
        c.wait()

    lane = lax.broadcasted_iota(jnp.int32, (ny, 128), 1)
    group = (lane * 43) >> 8
    inner = lane - G6 * group
    lane8, group8, inner8 = lane[0:8], group[0:8], inner[0:8]

    def lroll(a, s):
        s = s % 128
        return pltpu.roll(a, s, 1) if s else a


    def span_x(dx, deep):
        if dx == 0:
            return (2, 2, nx)
        if dx == 1:
            return (nx, 0, 2) if deep else (nx + 1, 1, 1)
        return (2, nx + 2, 2) if deep else (2, nx + 2, 1)

    def span_y(dy, deep):
        if dy == 0:
            return (2, 2, ny)
        if dy == 1:
            return (ny, 0, 2) if deep else (ny + 1, 1, 1)
        return (2, ny + 2, 2) if deep else (2, ny + 2, 1)

    def remote(src, dst, j, d):
        return pltpu.make_async_remote_copy(src_ref=src, dst_ref=dst, send_sem=send.at[j], recv_sem=recv.at[j], device_id=dev(d), device_id_type=MESH)

    def span_copy(n):
        dx, dy, dz = d = span_offsets[n]
        s = 1 if dz == 1 else 0
        ys, yd, yn = span_y(dy, True)
        return remote(PK.at[s, :, ys - 2 : ys - 2 + yn, :], R.at[s, 1 - dx, :, yd : yd + yn, :], n, d)

    def plane_copies(n, part=None):
        dx, dy = plane_offsets[n]
        d = (dx, dy, 0)
        base = len(span_offsets) + (2 * chunks + 1) * n
        out = []
        for c in range(chunks if dx == 0 else 1):
            if part is not None and c != part:
                continue
            for k in range(2):
                xs, xd, xn = span_x(dx, k == 0)
                if dx == 0:
                    xs, xd, xn = 2 + c * chunk, 2 + c * chunk, chunk
                ys, yd, yn = span_y(dy, k == 0)
                f0 = 3 * k
                out.append(remote(V.at[f0 : f0 + 3, :, xs : xs + xn, ys : ys + yn, :], V.at[f0 : f0 + 3, :, xd : xd + xn, yd : yd + yn, :], base + 2 * c + k, d))
        return out

    def edge_rows(n):
        dx, dy = plane_offsets[n]
        ys, yd, yn = span_y(dy, True)
        return remote(TE.at[:, :, ys : ys + yn, :], TE.at[:, :, yd : yd + yn, :], len(span_offsets) + (2 * chunks + 1) * n + 2 * chunks, (dx, dy, 0))

    everything = [(d, (lambda n=n: [span_copy(n)])) for n, d in enumerate(span_offsets)]
    everything += [((dx, dy, 0), (lambda n=n: plane_copies(n))) for n, (dx, dy) in enumerate(plane_offsets)]
    def send_all(wanted):
        for d, make in everything:
            if wanted(d):
                def go(make=make):
                    for c in make():
                        c.start()
                when(exists(d[0], d[1]), go)

    def send_chunk(c):
        for n, (dx, dy) in enumerate(plane_offsets):
            if dx == 0:
                def go(n=n):
                    for cp in plane_copies(n, c):
                        cp.start()
                when(exists(0, dy), go)

    send_chunk(0)
    for c in loads[1]:
        c.wait()
    for f in range(6):
        for s in range(2):
            acc = jnp.zeros((ny, 128), jnp.float32)
            for p in range(2, 2 + nx):
                tile = V[f, 0 if s == 0 else nt - 1, p, 2 : 2 + ny, :]
                acc = jnp.where(group == p, lroll(tile, G6 * p - (0 if s == 0 else 122)), acc)
            TE[s, f, 2 : 2 + ny, :] = acc
    for s in range(2):
        for k in range(2):
            parts = [lroll(TE[s, 3 * k + c, 2 : 2 + ny, :], 2 * c - (0 if s == 0 else 4)) for c in range(3)]
            PK[s, k] = jnp.where(inner < 2, parts[0], jnp.where(inner < 4, parts[1], parts[2]))

    for c in range(1, chunks):
        send_chunk(c)
    for n, (dx, dy) in enumerate(plane_offsets):
        if dx == 0:
            when(exists(dx, dy), lambda n=n: edge_rows(n).start())
    send_all(lambda d: d[2] == 0 and d[0] != 0)
    relay(1)
    relay(-1)
    send_all(lambda d: d[2] != 0)
    def land(wanted):
        for d, make in everything:
            if wanted(d):
                def arrive(make=make):
                    for c in make():
                        c.wait_recv()
                when(exists(-d[0], -d[1]), arrive)

    first, last = lane8 == 0, lane8 == 127

    def zup(a):
        r = [pltpu.roll(v, 127, 1) for v in a]
        return [jnp.where(last, r[(t + 1) % nt], r[t]) for t in range(nt)]

    def zdown(a):
        r = [pltpu.roll(v, 1, 1) for v in a]
        return [jnp.where(first, r[t - 1], r[t]) for t in range(nt)]

    def zsmooth(a):
        return [(v + v) + (w + q) for v, w, q in zip(a, zup(a), zdown(a))]

    def field_plane(x, _):
        for r in starts:
            here = slice(r, r + 8)
            m = [[V[3 + c, t, x, here, :] for c in range(3)] for t in range(nt)]
            u, d = [], [[[None] * 3 for _ in range(3)] for _ in range(nt)]
            for i in range(3):
                mid = [V[i, t, x, here, :] for t in range(nt)]
                u.append(mid)
                hi, lo = zup(mid), zdown(mid)
                for t in range(nt):
                    above, below = V[i, t, x, r + 1 : r + 9, :], V[i, t, x, r - 1 : r + 7, :]
                    Gv[i, t, x, here, :] = (mid[t] + mid[t]) + (above + below)
                    d[t][i][0] = m[t][0] * (V[i, t, x + 1, here, :] - V[i, t, x - 1, here, :])
                    d[t][i][1] = m[t][1] * (above - below)
                    d[t][i][2] = m[t][2] * (hi[t] - lo[t])
            for t in range(nt):
                f, square = tensor(d[t])
                mag = root(0.5 * square)
                dq = jnp.exp2((-2.0 / 3.0) * jnp.log2(m[t][0] * m[t][1] * m[t][2]))
                Q[t, x, here, :] = dq
                M[t, x, here, :] = dq * mag
                for k, (a, b) in enumerate(pairs):
                    F[k, t, x, here, :] = u[a][t] * u[b][t]
                    F[6 + k, t, x, here, :] = mag * f[k]
        return 0

    def velocity_plane(x, _):
        for c in range(3):
            for t in range(nt):
                for r in starts:
                    mid = V[c, t, x, r : r + 8, :]
                    Gv[c, t, x, r : r + 8, :] = (mid + mid) + (V[c, t, x, r - 1 : r + 7, :] + V[c, t, x, r + 1 : r + 9, :])
        return 0

    zi = lax.broadcasted_iota(jnp.int32, (nz, nz), 0)
    zj = lax.broadcasted_iota(jnp.int32, (nz, nz), 1)
    gap = jnp.abs(zi - zj)
    W[...] = jnp.where(gap == 0, 2.0, jnp.where((gap == 1) | (gap == nz - 1), 1.0, 0.0)).astype(jnp.bfloat16)

    gap = jnp.abs(zi[0:128, 0:128] - zj[0:128, 0:128])
    W2[...] = jnp.where(gap == 0, 4.0, jnp.where((gap == 1) | (gap == G6), 2.0, jnp.where((gap == G6 - 1) | (gap == G6 + 1), 1.0, 0.0))).astype(jnp.bfloat16)

    def banded(a, w):
        hi = a.astype(jnp.bfloat16)
        rest = a - hi.astype(jnp.float32)
        mid = rest.astype(jnp.bfloat16)
        low = (rest - mid.astype(jnp.float32)).astype(jnp.bfloat16)
        n = a.shape[0]
        out = jnp.dot(jnp.concatenate([hi, mid, low], axis=0), w, preferred_element_type=jnp.float32)
        return out[0:n] + (out[n : 2 * n] + out[2 * n :])

    def smooth_plane(x, _):
        for k0 in (0,):
            s = []
            for k in range(12):
                row = []
                for t in range(nt):
                    mid = F[k, t, x, 2 : 2 + ny, :]
                    row.append((mid + mid) + (F[k, t, x, 1 : 1 + ny, :] + F[k, t, x, 3 : 3 + ny, :]))
                s.append(jnp.concatenate(row, axis=1))
            s = banded(jnp.concatenate(s, axis=0), W[...])
            for k in range(12):
                for t in range(nt):
                    G[k, t, x, 0:ny, :] = s[(k - k0) * ny : (k - k0 + 1) * ny, 128 * t : 128 * t + 128]
        return 0

    has_lo = jnp.where(iy > 0, 0.125, 0.0)
    has_hi = jnp.where(iy < NY - 1, 0.125, 0.0)
    rows8 = lax.broadcasted_iota(jnp.int32, (8, 128), 0)

    def row_scale(r):
        idx = rows8 + r
        return jnp.where(idx < 2, has_lo, jnp.where(idx < ny + 2, 0.125, has_hi))

    def hat_plane(x, _):
        inside = jnp.where((x == 1) & (ix == 0), 0.0, jnp.where((x == nx + 2) & (ix == NX - 1), 0.0, 1.0))
        for r in starts:
            scale = row_scale(r) * inside
            for c in range(3):
                s = []
                for t in range(nt):
                    mid = Gv[c, t, x, r : r + 8, :]
                    s.append((mid + mid) + (Gv[c, t, x - 1, r : r + 8, :] + Gv[c, t, x + 1, r : r + 8, :]))
                s = zsmooth(s)
                for t in range(nt):
                    H[c, t, x, r : r + 8, :] = s[t] * scale
        return 0

    keep = [None] * nt
    keep[0] = lane8 >= 2
    keep[nt - 1] = (lane8 < 126) if nt > 1 else (lane8 >= 2) & (lane8 < 126)

    def line_plane(x, sums):
        out = []
        for b, r in enumerate(range(0, ny, 8)):
            here = slice(r + 2, r + 10)
            filtered = []
            for k in range(12):
                s = []
                for t in range(nt):
                    mid = G[k, t, x, r : r + 8, :]
                    s.append((mid + mid) + (G[k, t, x - 1, r : r + 8, :] + G[k, t, x + 1, r : r + 8, :]))
                filtered.append(s)
            hat, d = [], [[[None] * 3 for _ in range(3)] for _ in range(nt)]
            m = [[V[3 + c, t, x, here, :] for c in range(3)] for t in range(nt)]
            for i in range(3):
                mid = [H[i, t, x, here, :] for t in range(nt)]
                hat.append(mid)
                hi, lo = zup(mid), zdown(mid)
                for t in range(nt):
                    d[t][i][0] = m[t][0] * (H[i, t, x + 1, here, :] - H[i, t, x - 1, here, :])
                    d[t][i][1] = m[t][1] * (H[i, t, x, r + 3 : r + 11, :] - H[i, t, x, r + 1 : r + 9, :])
                    d[t][i][2] = m[t][2] * (hi[t] - lo[t])
            num = den = 0.0
            for t in range(nt):
                n, e = model_sums([filtered[k][t] for k in range(6)], [filtered[6 + k][t] for k in range(6)], [h[t] for h in hat], d[t], Q[t, x, here, :])
                if keep[t] is not None:
                    n, e = jnp.where(keep[t], n, 0.0), jnp.where(keep[t], e, 0.0)
                num, den = num + n, den + e
            num = jnp.sum(num, axis=1, keepdims=True)
            den = jnp.sum(den, axis=1, keepdims=True)
            acc = jnp.where(lane8 == G6 * x + 2, num, sums[b])
            out.append(jnp.where(lane8 == G6 * x + 4, den, acc))
        return tuple(out)

    def land_chunk(c):
        for n, (dx, dy) in enumerate(plane_offsets):
            if dx == 0:
                def arrive(n=n):
                    for cp in plane_copies(n, c):
                        cp.wait_recv()
                when(exists(0, -dy), arrive)

    def land_x():
        land(lambda d: d[0] != 0 and d[2] == 0)

    def order(i):
        i = jnp.clip(i, 0, nx + 1)
        return jnp.where(i < nx, i + 3, nx + 2 - i)

    def line_order(i):
        i = jnp.clip(i, 0, nx - 1)
        return jnp.where(i < nx - 2, i + 4, nx + 1 - i)

    def step(i, sums):
        sums = line_plane(line_order(i - 5), sums)
        hat_plane(order(i - 2), 0)
        smooth_plane(order(i - 1), 0)
        field_plane(order(i), 0)
        return sums

    def land_far():
        land_x()
        for p in (0, nx + 3):
            velocity_plane(p, 0)

    waits = [(chunk * c - 2, functools.partial(land_chunk, c)) for c in range(1, chunks)] + [(nx - 2, land_far)]
    sums = tuple(jnp.zeros((8, 128), jnp.float32) for _ in range(0, ny, 8))

    def turn(j, sums):
        def arrivals():
            for at, wait in waits:
                pl.when(j == at)(wait)
        pl.when(lax.rem(j + 2, chunk) == 0)(arrivals)
        return step(j, sums)
    land_chunk(0)
    velocity_plane(2, 0)
    sums = lax.fori_loop(0, nx + 5, turn, sums)
    land(lambda d: d[2] != 0)
    for n, (dx, dy) in enumerate(plane_offsets):
        if dx == 0:
            when(exists(dx, -dy), lambda n=n: edge_rows(n).wait_recv())

    yr = ny + 8
    lane_r = lax.broadcasted_iota(jnp.int32, (yr, 128), 1)
    group_r = (lane_r * 43) >> 8
    inner_r = lane_r - G6 * group_r
    rows_r = lax.broadcasted_iota(jnp.int32, (yr, 128), 0)
    outside = ((group_r == 1) & (ix == 0)) | ((group_r == nx + 2) & (ix == NX - 1))
    outside = outside | ((rows_r < 2) & (iy == 0)) | ((rows_r >= ny + 2) & (iy == NY - 1))
    scale_r = jnp.where(outside, 0.0, 0.125)
    enum, eden = 0.0, 0.0
    fixes = []
    for s in range(2):
        mixed = []
        for k in range(2):
            far = jnp.where(lane_r < 2 * G6, lroll(R[1 - s, 0, k], -G6 * nx), R[1 - s, 1, k])
            mixed.append(jnp.where(lane_r >= G6 * (nx + 2), lroll(R[1 - s, 2, k], G6 * nx), far))
        fields = []
        for f in range(6):
            own = TE[s, f]
            for p in (0, 1, nx + 2, nx + 3):
                if f >= 3 and p in (0, nx + 3):
                    continue
                tile = V[f, 0 if s == 0 else nt - 1, p]
                own = jnp.where(group_r == p, lroll(tile, G6 * p - (0 if s == 0 else 122)), own)
            c = f % 3
            if s == 0:
                fields.append(jnp.where(inner_r < 2, lroll(mixed[f // 3], -2 * c), lroll(own, 2)))
            else:
                fields.append(jnp.where(inner_r >= 4, lroll(mixed[f // 3], 4 - 2 * c), lroll(own, -2)))
        u, m = fields[0:3], fields[3:6]
        for f in range(6):
            E[s, f] = fields[f]
        def shift(a, n):
            return lroll(a, -n)
        d = [[None] * 3 for _ in range(3)]
        for i in range(3):
            d[i][0] = m[0] * (shift(u[i], G6) - shift(u[i], -G6))
            d[i][1] = m[1] * (pltpu.roll(u[i], yr - 1, 0) - pltpu.roll(u[i], 1, 0))
            d[i][2] = m[2] * (shift(u[i], 1) - shift(u[i], -1))
        f, square = tensor(d)
        mag = root(0.5 * square)
        dq = jnp.exp2((-2.0 / 3.0) * jnp.log2(m[0] * m[1] * m[2]))
        EF[s, 15] = dq
        EF[s, 16] = dq * mag
        for c in range(3):
            EF[s, 12 + c] = u[c]
        for k, (a, b) in enumerate(pairs):
            EF[s, k] = u[a] * u[b]
            EF[s, 6 + k] = mag * f[k]
        rows = []
        for c in range(3):
            rows.append((u[c] + u[c]) + (pltpu.roll(u[c], yr - 1, 0) + pltpu.roll(u[c], 1, 0)))
        own = slice(2, 2 + ny)
        for k in range(12):
            mid = EF[s, k, own, :]
            rows.append((mid + mid) + (EF[s, k, 1 : 1 + ny, :] + EF[s, k, 3 : 3 + ny, :]))
        smoothed = banded(jnp.concatenate(rows, axis=0), W2[...])
        for c in range(3):
            EG[s, c] = smoothed[yr * c : yr * (c + 1)] * scale_r
        filtered = [smoothed[3 * yr + ny * k : 3 * yr + ny * (k + 1)] for k in range(12)]
        hat, dh = [], [[None] * 3 for _ in range(3)]
        me = [E[s, 3 + c, own, :] for c in range(3)]
        for i in range(3):
            mid = EG[s, i, own, :]
            hat.append(mid)
            dh[i][0] = me[0] * (shift(mid, G6) - shift(mid, -G6))
            dh[i][1] = me[1] * (EG[s, i, 3 : 3 + ny, :] - EG[s, i, 1 : 1 + ny, :])
            dh[i][2] = me[2] * (shift(mid, 1) - shift(mid, -1))
        n, e = model_sums(filtered[0:6], filtered[6:12], hat, dh, EF[s, 15, own, :])
        enum, eden = enum + n, eden + e
    enum = enum + lroll(enum, -1)
    eden = lroll(eden + lroll(eden, -1), 2)
    used = (group >= 2) & (group < nx + 2)
    extra = jnp.where(used & (inner == 2), enum, jnp.where(used & (inner == 4), eden, 0.0))
    LS[iz] = jnp.concatenate(sums, axis=0) + extra

    def line_copy(o):
        return pltpu.make_async_remote_copy(
            src_ref=LS.at[iz], dst_ref=LS.at[iz], send_sem=lsend.at[o - 1], recv_sem=lrecv.at[o - 1],
            device_id=(ix, iy, lax.rem(iz + o, NZ)), device_id_type=MESH)
    def line_landing(o):
        src = lax.rem(iz - o + NZ, NZ)
        return pltpu.make_async_remote_copy(
            src_ref=LS.at[src], dst_ref=LS.at[src], send_sem=lsend.at[o - 1], recv_sem=lrecv.at[o - 1],
            device_id=(ix, iy, lax.rem(iz + o, NZ)), device_id_type=MESH)
    for o in range(1, NZ):
        line_copy(o).start()

    lo_fix, hi_fix = EF[0, 16, 2 : 2 + ny, :], EF[1, 16, 2 : 2 + ny, :]
    def weight_plane(x, _):
        p = x + 2
        for t in range(nt):
            tile = M[t, p, 2 : 2 + ny, :]
            if t == 0:
                tile = jnp.where(lane == 0, pltpu.roll(lo_fix, 126 - G6 * p, 1), tile)
            if t == nt - 1:
                tile = jnp.where(lane == 127, pltpu.roll(hi_fix, 124 - G6 * p, 1), tile)
            D[x, :, 128 * t : 128 * t + 128] = tile
        return 0
    lax.fori_loop(0, nx, weight_plane, 0, unroll=4)
    for o in range(1, NZ):
        line_landing(o).wait_recv()
    total = LS[0]
    for o in range(1, NZ):
        total = total + LS[o]
    unit = 4096.0 * nz * NZ
    coef = (total / unit) / (lroll(total, -2) / unit + eps_line)
    masked = jnp.where(used & (inner == 2), coef, -jnp.inf)
    here_max = masked[0:8]
    for r in range(8, ny, 8):
        here_max = jnp.maximum(here_max, masked[r : r + 8])
    me = ix * NY + iy
    PS[me] = here_max
    def peak_copy(j, a, b, landing):
        tx, ty = lax.rem(ix + a, NX), lax.rem(iy + b, NY)
        slot = me
        if landing:
            slot = lax.rem(ix - a + NX, NX) * NY + lax.rem(iy - b + NY, NY)
        return pltpu.make_async_remote_copy(
            src_ref=PS.at[slot], dst_ref=PS.at[slot], send_sem=psend.at[j], recv_sem=precv.at[j],
            device_id=(tx, ty, iz), device_id_type=MESH)
    for j, (a, b) in enumerate(plane_peers):
        peak_copy(j, a, b, False).start()
    table = coef.T
    for x in range(nx):
        at = G6 * (x + 2) + 2
        cols[x] = jnp.broadcast_to(jnp.sum(jnp.where(lane == at, coef, 0.0), axis=1, keepdims=True), (ny, 128))
        turned[x : x + 1, :] = table[at : at + 1, :]
    for o in range(1, NZ):
        line_copy(o).wait_send()
    for d, make in everything:
        def left(make=make):
            for c in make():
                c.wait_send()
        when(exists(d[0], d[1]), left)
    for n, (dx, dy) in enumerate(plane_offsets):
        if dx == 0:
            when(exists(dx, dy), lambda n=n: edge_rows(n).wait_send())
    for j, (a, b) in enumerate(plane_peers):
        peak_copy(j, a, b, True).wait_recv()
    peak = PS[0]
    for j in range(1, NX * NY):
        peak = jnp.maximum(peak, PS[j])
    half[...] = jnp.broadcast_to(0.5 * jnp.max(peak, axis=(0, 1), keepdims=True), (8, 128))
    for j, (a, b) in enumerate(plane_peers):
        peak_copy(j, a, b, False).wait_send()


def scale_kernel(D, cols, turned, half, visc, coef_out):
    nx, ny, nz = visc.shape
    limit = half[0:1, :]
    for x in range(nx):
        column = jnp.minimum(cols[x], limit)
        for t in range(0, nz, 128):
            visc[x, :, t : t + 128] = D[x, :, t : t + 128] * column
    coef_out[...] = jnp.minimum(turned[...], limit[:, 0:ny])


def per_device(sizes, velocity, metric):
    nx, ny, nz = velocity.shape[1:]
    NX, NY, NZ = sizes
    assert nz % 128 == 0 and ny % 8 == 0 and G6 * (nx + 4) <= 128 and nx >= 6
    nt, pa, yr = nz // 128, nx + 4 + (nx + 1) % 2, ny + 8
    f32 = jnp.float32
    copies = len(span_offsets) + (2 * chunks + 1) * len(plane_offsets)
    parts = pl.pallas_call(
        functools.partial(kernel, sizes),
        out_shape=(pltpu.VMEM((nx, ny, nz), f32), pltpu.VMEM((nx, ny, 128), f32), pltpu.VMEM((nx, ny), f32), pltpu.VMEM((8, 128), f32)),
        in_specs=[pl.BlockSpec(memory_space=pltpu.HBM)] * 2,
        out_specs=(pl.BlockSpec(memory_space=pltpu.VMEM),) * 4,
        scratch_shapes=[
            pltpu.VMEM((6, nt, pa, yr, 128), f32),
            pltpu.VMEM((3, nt, pa, yr, 128), f32),
            pltpu.VMEM((12, nt, pa, yr, 128), f32),
            pltpu.VMEM((3, nt, pa, yr, 128), f32),
            pltpu.VMEM((nt, pa, yr, 128), f32),
            pltpu.VMEM((nt, pa, yr, 128), f32),
            pltpu.VMEM((12, nt, pa, yr, 128), f32),
            pltpu.VMEM((2, 6, yr, 128), f32),
            pltpu.VMEM((2, 6, yr, 128), f32),
            pltpu.VMEM((2, 17, yr, 128), f32),
            pltpu.VMEM((2, 3, yr, 128), f32),
            pltpu.VMEM((2, 2, ny, 128), f32),
            pltpu.VMEM((2, 3, 2, yr, 128), f32),
            pltpu.VMEM((NZ, ny, 128), f32),
            pltpu.VMEM((NX * NY, 8, 128), f32),
            pltpu.VMEM((nz, nz), jnp.bfloat16),
            pltpu.VMEM((128, 128), jnp.bfloat16),
            pltpu.SemaphoreType.REGULAR((2,)),
            pltpu.SemaphoreType.DMA((4 * nt,)),
            pltpu.SemaphoreType.DMA((copies,)),
            pltpu.SemaphoreType.DMA((copies,)),
            pltpu.SemaphoreType.DMA((NZ,)),
            pltpu.SemaphoreType.DMA((NZ,)),
            pltpu.SemaphoreType.DMA((NX * NY,)),
            pltpu.SemaphoreType.DMA((NX * NY,)),
        ],
        compiler_params=pltpu.CompilerParams(collective_id=0, has_side_effects=True, vmem_limit_bytes=67043328 - 700 * 1024),
    )(velocity, metric)
    return pl.pallas_call(
        scale_kernel,
        out_shape=(jax.ShapeDtypeStruct((nx, ny, nz), f32), jax.ShapeDtypeStruct((nx, ny), f32)),
        in_specs=[pl.BlockSpec(memory_space=pltpu.VMEM)] * 4,
        out_specs=(pl.BlockSpec(memory_space=pltpu.VMEM),) * 2,
        compiler_params=pltpu.CompilerParams(vmem_limit_bytes=4 * 1024 * 1024),
    )(*parts)


def solution(mesh):
    sizes = (mesh.shape["gx"], mesh.shape["gy"], mesh.shape["gz"])
    return jax.shard_map(
        functools.partial(per_device, sizes),
        mesh=mesh,
        in_specs=(P(None, "gx", "gy", "gz"), P(None, "gx", "gy", "gz")),
        out_specs=(P("gx", "gy", "gz"), P("gx", "gy")),
        check_vma=False,
    )
```
